32 devices in a mesh: head: 2 (over x), inner: 4 (over y, core), outer: 4 (over z).
Axes of the slice: x: 2, y: 2, z: 4, core: 2. Of those that a mesh axis runs over, the one named last changes fastest.
Arguments:
- queries: float32 [2048, 8, 128], P(('inner', 'outer'), 'head'), may hold values from -8 to 8
- key_rows: float32 [2048, 128], P(('inner', 'outer'), 'head'), may hold values from -8 to 8
- values: float32 [2048, 128], P(('inner', 'outer'), 'head'), may hold values from -24 to 24
- out_grad: float32 [2048, 8, 128], P(('inner', 'outer'), 'head'), may hold values from -48 to 48
- sink_len: int32 [1], replicated, may hold values from 32 to 128
- window_len: int32 [1], replicated, may hold values from 129 to 640
- block_codes: int32 [16, 5], replicated, may hold values from 0 to 2, as said below
Outputs:
- query_grad: float32 [2048, 8, 128], P(('inner', 'outer'), 'head')
- key_grad: float32 [2048, 128], P(('inner', 'outer'), 'head')
- value_grad: float32 [2048, 128], P(('inner', 'outer'), 'head')
The draws below stay inside these ranges and needn't reach their ends.
Inputs may be any that keep to these rules, and one draw needn't show every extreme that they name: block_codes[b, 0] is 1 or 2 for every block b.
All inputs are finite; a program needn't handle non-finite values.
Results may differ from the reference program's by a relative error of at most 0.0003.
Values sent between devices are 32-bit elements; how exact they have to be, the bound alone decides.
A program may use at most 64 MiB of HBM per device.

```python
import math
import jax
import jax.numpy as jnp
from jax import lax

HEAD_DIM = 128
TOK_DEV = 128
STEPS = 5
SINK = 128
NSEQ = 16
TOKENS = 2048
HEADS = 8
KV_HEADS = 1


def paired_draw(key):
    base = jax.random.fold_in(key, 77)
    query_key, key_key = jax.random.split(base, 2)
    queries = jax.random.normal(query_key, (TOKENS, HEADS, HEAD_DIM), jnp.float32)
    key_heads = jax.random.normal(key_key, (TOKENS, KV_HEADS, HEAD_DIM), jnp.float32)
    queries = jnp.clip(queries, -8.0, 8.0)
    key_heads = jnp.clip(key_heads, -8.0, 8.0)
    return (queries, key_heads.reshape(TOKENS, KV_HEADS * HEAD_DIM))


def draw_queries(key, part):
    return paired_draw(key)[0]


def draw_key_rows(key, part):
    return paired_draw(key)[1]


def draw_block_codes(key, part):
    others = jax.random.randint(key, (NSEQ, STEPS), 0, 3, dtype=jnp.int32)
    leading = jax.random.randint(jax.random.fold_in(key, 5), (NSEQ, 1), 1, 3, dtype=jnp.int32)
    return jnp.concatenate([leading, others[:, 1:]], axis=1)


def block_levels(own_key, shape, shards, smallest, high):
    gain, own = 1.0, jax.random.fold_in(own_key, 6)
    for position, blocks in shards:
        steps = jnp.exp(jax.random.uniform(jax.random.fold_in(own, position), (blocks,), jnp.float32, smallest / len(shards), high / len(shards)))
        gain = gain * jnp.repeat(steps, shape[position] // blocks).reshape([-1 if axis == position else 1 for axis in range(len(shape))])
    return gain


def bell_draw(key, shape, width, most, shards=(), kind=jnp.bfloat16):
    result = width * jax.random.normal(key, shape, jnp.float32)
    if shards:
        result = result * block_levels(key, shape, shards, -0.22, 0.18)
    return jnp.clip(result, -most, most).astype(kind)


def setup_inputs(seed: int = 0) -> dict:
    seeds = jax.random.split(jax.random.key(seed), 8)
    return {
        "queries": draw_queries(jax.random.fold_in(seeds[7], 71), 0),
        "key_rows": draw_key_rows(jax.random.fold_in(seeds[7], 71), 0),
        "values": bell_draw(seeds[2], (TOKENS, KV_HEADS * HEAD_DIM), 4.0, 24.0, ((0, 16), (1, 2)), jnp.float32),
        "out_grad": bell_draw(seeds[3], (TOKENS, HEADS, HEAD_DIM), 8.0, 48.0, ((0, 16), (1, 2)), jnp.float32),
        "sink_len": jax.random.randint(seeds[4], (1,), SINK // 4, SINK + 1).astype(jnp.int32),
        "window_len": jax.random.randint(seeds[5], (1,), TOK_DEV + 1, STEPS * TOK_DEV + 1).astype(jnp.int32),
        "block_codes": draw_block_codes(jax.random.fold_in(seeds[7], 71), 0),
    }


very_low = -1e+30
precise = lax.Precision.HIGHEST

def reference(queries, key_rows, values, out_grad, sink_len, window_len, block_codes):
    group = HEADS // KV_HEADS
    temper = 1.0 / math.sqrt(HEAD_DIM)
    front_pad = (STEPS - 1) * TOK_DEV
    span = STEPS * TOK_DEV
    key_heads = key_rows.reshape(TOKENS, KV_HEADS, HEAD_DIM)
    value_heads = values.reshape(TOKENS, KV_HEADS, HEAD_DIM)
    padding = jnp.zeros((front_pad, KV_HEADS, HEAD_DIM), key_rows.dtype)
    padded_keys = jnp.concatenate([padding, key_heads], 0)
    padded_values = jnp.concatenate([padding, value_heads], 0)
    sink_keys = key_heads[:SINK]
    sink_values = value_heads[:SINK]
    sink_end = sink_len[0]
    window = window_len[0]
    local_ids = jnp.arange(TOK_DEV, dtype=jnp.int32)
    spread = jnp.arange(span, dtype=jnp.int32)
    sink_ids = jnp.arange(SINK, dtype=jnp.int32)

    def one_block(carry, query_block):
        grad_keys, grad_values, sink_dk, sink_dv = carry
        start = (query_block * TOK_DEV).astype(jnp.int32)
        query_blk = lax.dynamic_slice_in_dim(queries, start, TOK_DEV, 0).reshape(TOK_DEV, KV_HEADS, group, HEAD_DIM)
        grad_blk = lax.dynamic_slice_in_dim(out_grad, start, TOK_DEV, 0).reshape(TOK_DEV, KV_HEADS, group, HEAD_DIM)
        window_keys = lax.dynamic_slice_in_dim(padded_keys, start, span, 0)
        window_values = lax.dynamic_slice_in_dim(padded_values, start, span, 0)
        all_keys = jnp.concatenate([sink_keys, window_keys], 0)
        all_values = jnp.concatenate([sink_values, window_values], 0)
        pos_q = start + local_ids
        pos_k = start - front_pad + spread
        offsets = (STEPS - 1 - spread // TOK_DEV).astype(jnp.int32)
        code_row = lax.dynamic_index_in_dim(block_codes, query_block, 0, keepdims=False)
        codes = code_row[offsets]
        rule = (codes != 0)[None, :] & ((codes == 2)[None, :] | (pos_q[:, None] - pos_k[None, :] < window))
        in_sink = (pos_k < sink_end)[None, :]
        chosen = jnp.where(query_block == 0, in_sink | rule, jnp.logical_not(in_sink) & rule)
        seen_window = (pos_k >= 0)[None, :] & (pos_k[None, :] <= pos_q[:, None]) & chosen
        seen_sink = jnp.broadcast_to(((query_block >= 1) & (sink_ids < sink_end))[None, :], (TOK_DEV, SINK))
        allowed = jnp.concatenate([seen_sink, seen_window], 1)
        logits = temper * jnp.einsum('tkgd,skd->kgts', query_blk, all_keys, precision=precise)
        logits = jnp.where(allowed, logits, very_low)
        row_max = lax.optimization_barrier(jnp.max(logits, axis=3, keepdims=True))
        weights = jnp.where(allowed, jnp.exp(logits - row_max), 0.0)
        probs = weights / lax.optimization_barrier(jnp.sum(weights, axis=3, keepdims=True))
        attended = jnp.einsum('kgts,skd->tkgd', probs, all_values, precision=precise)
        row_delta = jnp.einsum('tkgd,tkgd->kgt', grad_blk, attended, precision=precise)
        grad_dots = jnp.einsum('tkgd,skd->kgts', grad_blk, all_values, precision=precise)
        dscores = probs * (grad_dots - row_delta[..., None])
        step_dq = temper * jnp.einsum('kgts,skd->tkgd', dscores, all_keys, precision=precise)
        step_dk = temper * jnp.einsum('kgts,tkgd->skd', dscores, query_blk, precision=precise)
        step_dv = jnp.einsum('kgts,tkgd->skd', probs, grad_blk, precision=precise)
        current_k = lax.dynamic_slice_in_dim(grad_keys, start, span, 0)
        grad_keys = lax.dynamic_update_slice_in_dim(grad_keys, current_k + step_dk[SINK:], start, 0)
        current_v = lax.dynamic_slice_in_dim(grad_values, start, span, 0)
        grad_values = lax.dynamic_update_slice_in_dim(grad_values, current_v + step_dv[SINK:], start, 0)
        sink_dk = sink_dk + step_dk[:SINK]
        sink_dv = sink_dv + step_dv[:SINK]
        return ((grad_keys, grad_values, sink_dk, sink_dv), step_dq.reshape(TOK_DEV, HEADS, HEAD_DIM))
    zero_grads = jnp.zeros((front_pad + TOKENS, KV_HEADS, HEAD_DIM), queries.dtype)
    zero_sink = jnp.zeros((SINK, KV_HEADS, HEAD_DIM), queries.dtype)
    carry, stacked = lax.scan(one_block, (zero_grads, zero_grads, zero_sink, zero_sink), jnp.arange(NSEQ, dtype=jnp.int32))
    grad_keys, grad_values, sink_dk, sink_dv = carry
    key_grad = grad_keys[front_pad:].at[:SINK].add(sink_dk)
    value_grad = grad_values[front_pad:].at[:SINK].add(sink_dv)
    query_grad = stacked.reshape(TOKENS, HEADS, HEAD_DIM)
    return (query_grad, key_grad.reshape(TOKENS, KV_HEADS * HEAD_DIM), value_grad.reshape(TOKENS, KV_HEADS * HEAD_DIM))
```

```python
import functools
import math

import jax
import jax.numpy as jnp
from jax import lax
from jax.experimental import pallas as pl
from jax.experimental.pallas import tpu as pltpu
from jax.sharding import PartitionSpec as P

STEPS = 5
FAR = STEPS - 1
BIG = 1 << 28
very_low = -1e30
f32, bf16 = jnp.float32, jnp.bfloat16
MESH = pl.DeviceIdType.MESH
NT = (((1,), (1,)), ((), ()))
NN = (((1,), (0,)), ((), ()))


def dot(a, b, dims):
    return lax.dot_general(a, b, dims, preferred_element_type=f32)


def two(x):
    hi = x.astype(bf16)
    return hi, (x - hi.astype(f32)).astype(bf16)


def when(cond, f):
    if cond is None:
        f()
    else:
        pl.when(cond)(f)


def kernel(
    sizes, sink_hbm, window_hbm, codes_hbm, q_hbm, k_hbm, v_hbm, g_hbm, dq_ref, dkv_ref,
    sink_ref, window_ref, codes_ref, q_ref, g_ref, load, buf, sinkb, piece, qcat, gcat,
    st, dp, peak, run, ds, ktcat, xout, xin, mine, gout, gin, g4out, g4in, sg, sin, s2, s2in,
    dqt, send, recv,
):
    ni, no, heads_dev = sizes
    half, block = k_hbm.shape
    rows = q_ref.shape[0]
    temper = 1.0 / math.sqrt(2 * half)
    head, inner, outer = lax.axis_index("head"), lax.axis_index("inner"), lax.axis_index("outer")
    par = lax.rem(head, 2)
    other = 1 - par
    partner = head + 1 - 2 * par
    count = ni * no
    b = inner * no + outer
    pr = block // ni

    def seq(o):
        t = lax.rem(b + o + count, count)
        return (head, t // no, lax.rem(t, no))

    across = (partner, inner, outer)
    columns = [(p, d) for p in range(2) for d in range(ni) if p or d]
    first = (inner == 0) & (outer == 0)
    top = outer == 0

    def column(p, d):
        return (partner if p else head, lax.rem(inner + d, ni), outer)

    def up(o):
        return b + o < count

    def down(o):
        return b >= o

    slots = {}

    def sem(name):
        return slots.setdefault(name, len(slots))

    pending = []

    def copy(name, src, dst, device):
        return pltpu.make_async_remote_copy(
            src_ref=src, dst_ref=dst, send_sem=send.at[sem(name)], recv_sem=recv.at[sem(name)],
            device_id=device, device_id_type=MESH,
        )

    def start(name, src, dst, device, cond=None, sent=True):
        c = copy(name, src, dst, device)
        when(cond, c.start)
        if sent:
            pending.append((cond, c))

    def sent(name, like, cond=None):
        pending.append((cond, copy(name, like, like, across)))

    def arrived(name, dst):
        copy(name, dst, dst, across).wait_recv()

    moves = [
        (k_hbm, buf.at[0, par, 0:half]), (v_hbm, buf.at[0, par, half:2 * half]),
        (q_hbm, q_ref), (g_hbm, g_ref),
        (codes_hbm, codes_ref), (sink_hbm, sink_ref), (window_hbm, window_ref),
    ]
    loads = [pltpu.make_async_copy(x, y, load.at[i]) for i, (x, y) in enumerate(moves)]

    barrier = pltpu.get_barrier_semaphore()

    def greet(device):
        pl.semaphore_signal(barrier, inc=1, device_id=device, device_id_type=MESH)

    for p, d in columns:
        greet(column(p, d))
    expect = len(columns)
    for o in range(1, STEPS):
        when(up(o), lambda: greet(seq(o)))
        when(down(o), lambda: greet(seq(-o)))
        expect = expect + up(o).astype(jnp.int32) + down(o).astype(jnp.int32)
    when(outer != 0, lambda: greet((head, inner, 0)))
    expect = expect + jnp.where(top, no - 1, 0) + jnp.where(first, 0, 1)

    @pl.when(first)
    def _():
        for i in range(ni):
            for z in range(no):
                if i or z:
                    greet((head, i, z))

    for x in loads:
        x.start()
    pl.semaphore_wait(barrier, expect)

    def own_to(name, o, dst, device, cond=None):
        start(name, k_hbm, dst.at[0:half], device, cond, False)
        start(name, v_hbm, dst.at[half:2 * half], device, cond, False)
        sent(name, dst, cond)

    def rows_of(i):
        return (k_hbm.at[pl.ds(i * pr, pr)] if i * pr < half
                else v_hbm.at[pl.ds(i * pr - half, pr)])

    for i in range(ni):
        for p in range(2):
            if i or p:
                to = (partner if p else head, i, 0)
                start(f"f1_{p}", rows_of(i), piece.at[par], to, first, False)
    sent("f1_0", buf.at[0, 0, 0:(ni - 1) * pr], first)
    sent("f1_1", buf.at[0, 0], first)

    own_to("x0", 0, buf.at[0, par], across)
    for o in (3, 2, 1, 4):
        own_to(f"w{o}", o, buf.at[o, par], seq(o), up(o))

    loads[2].wait()
    q0, q1 = two(q_ref[...])
    qcat[...] = jnp.concatenate([q0, q1], 1)
    loads[3].wait()
    g0, g1 = two(g_ref[...])
    gcat[...] = jnp.concatenate([g0, g1], 1)
    for i in (0, 1, 4, 5, 6):
        loads[i].wait()

    @pl.when(first)
    def _():
        piece[par] = buf[0, par, 0:pr, :]

    jk = lax.broadcasted_iota(jnp.int32, (block, rows), 0)
    iq = lax.broadcasted_iota(jnp.int32, (block, rows), 1) // heads_dev
    gap = iq - jk
    sink_end, window = sink_ref[0], window_ref[0]

    def mask_of(o):
        code = codes_ref[o, b]
        limit = jnp.where(code == 2, BIG, jnp.where(code == 1, window, -BIG)) - o * block
        here = jnp.where(b == o, sink_end, 0)
        if o == 0:
            return (gap >= 0) & ((gap < limit) | (jk < here))
        return (gap < limit) & (jk >= here)

    def scores_of(keys, vals, index, allowed):
        k0, k1 = two(keys.T)
        v0, v1 = two(vals.T)
        kk = jnp.concatenate([jnp.concatenate([k0, k0], 1), jnp.concatenate([k1, k1], 1)], 0)
        vv = jnp.concatenate([jnp.concatenate([v0, v0], 1), jnp.concatenate([v1, v1], 1)], 0)
        s = dot(kk, qcat[...], NT)
        s = jnp.where(allowed, temper * (s[0:block] + s[block:]), very_low)
        d = dot(vv, gcat[...], NT)
        d = d[0:block] + d[block:]
        t0, t1 = two(keys * temper)
        ktcat[index] = jnp.concatenate([t0, t1, t0], 1)
        high = jnp.max(s, axis=0, keepdims=True)
        if index:
            before = run[0:1]
            high = jnp.maximum(high, before)
            shrink = jnp.exp(before - high)
        e = jnp.exp(s - high)
        st[index] = e
        dp[index] = d
        norm = jnp.sum(e, axis=0, keepdims=True)
        delta = jnp.sum(e * d, axis=0, keepdims=True)
        if index:
            norm = norm + shrink * run[1:2]
            delta = delta + shrink * run[2:3]
        peak[index:index + 1] = high
        run[0:1] = high
        run[1:2] = norm
        run[2:3] = delta

    def slot(o):
        def _():
            a, c = buf[o, 0], buf[o, 1]
            scores_of(
                jnp.concatenate([a[0:half], c[0:half]], 0),
                jnp.concatenate([a[half:], c[half:]], 0), o, mask_of(o),
            )
        return _

    @pl.when(top)
    def _():
        @pl.when(jnp.logical_not(first))
        def _():
            arrived("f1_0", piece.at[par])
        arrived("f1_1", piece.at[other])
    for z in range(1, no):
        start("f2", piece, piece, (head, inner, z), top, False)
    sent("f2", sinkb.at[0:no - 1], top)

    arrived("x0", buf.at[0, other])
    start("w4x", buf.at[0, other], buf.at[FAR, other], seq(FAR), up(FAR))
    slot(0)()

    def relay(o):
        def _():
            arrived(f"w{o}", buf.at[o, par])
            copy(f"r{o}", buf.at[o, par], buf.at[o, par], across).start()
        when(down(o), _)

    def relays(order):
        def _():
            for o in order:
                relay(o)
        return _

    near = list(range(1, FAR))
    when(outer == 0, relays(near[::-1]))
    when(outer == no - 1, relays(near))
    when((outer != 0) & (outer != no - 1), relays(near[::2] + near[1::2]))
    for o in near:
        pending.append((down(o), copy(f"r{o}", buf.at[o, par], buf.at[o, par], across)))

    @pl.when(outer != 0)
    def _():
        arrived("f2", piece)
    for d in range(1, ni):
        start("f3", piece, sinkb.at[inner], column(0, d), None, False)
    sent("f3", sinkb.at[0:ni - 1])
    sinkb[inner] = piece[...]

    @pl.when(down(FAR))
    def _():
        arrived(f"w{FAR}", buf.at[FAR, par])
        arrived("w4x", buf.at[FAR, other])
        slot(FAR)()

    for o in near:
        @pl.when(down(o))
        def _():
            arrived(f"r{o}", buf.at[o, other])
            slot(o)()

    arrived("f3", sinkb.at[0:ni - 1])

    @pl.when(b >= 1)
    def _():
        a = [sinkb[i, p] for p in range(2) for i in range(ni)]
        cut = ni // 2
        keys = jnp.concatenate(a[0:cut] + a[ni:ni + cut], 0)
        vals = jnp.concatenate(a[cut:ni] + a[ni + cut:], 0)
        scores_of(keys, vals, STEPS, jk < sink_end)

    high = run[0:1]
    scale = 1.0 / run[1:2]
    delta = run[2:3] * scale

    def grads(i):
        probs = st[i] * (jnp.exp(peak[i:i + 1] - high) * scale)
        score = probs * (dp[i] - delta)
        p_hi, p_lo = two(probs)
        d_hi, d_lo = two(score)
        ds[i, 0] = d_hi
        ds[i, 1] = d_lo
        w = 2 * half
        pv = dot(jnp.concatenate([p_hi, p_lo], 0), gcat[...], NN)
        dv = pv[0:block, 0:w] + pv[0:block, w:] + pv[block:, 0:w]
        kq = dot(jnp.concatenate([d_hi, d_lo], 0), qcat[...], NN)
        dk = temper * (kq[0:block, 0:w] + kq[0:block, w:] + kq[block:, 0:w])
        dk, dv = dk.T, dv.T
        even = jnp.concatenate([dk[0:half], dv[0:half]], 0)
        odd = jnp.concatenate([dk[half:], dv[half:]], 0)
        keep = jnp.where(par == 0, even, odd)
        give = jnp.where(par == 0, odd, even)
        return keep, give

    @pl.when(b >= 1)
    def _():
        keep, give = grads(STEPS)
        sg[0] = keep
        sg[1] = give

    @pl.when(b == 0)
    def _():
        sg[...] = jnp.zeros_like(sg)

    for p, d in columns:
        target = lax.rem(inner + d, ni)
        rng = pl.ds(pl.multiple_of(target * pr, pr), pr)
        start("b1", sg.at[p, rng], sin.at[p * ni + d], column(p, d), None, False)
    sent("b1", sin.at[1:2 * ni])

    def give_near(o):
        @pl.when(down(o))
        def _():
            keep, give = grads(o)
            mine[o] = keep
            xout[o] = give
        start(f"gx{o}", xout.at[o], xin.at[o], across, down(o))

    def pass_on(o):
        @pl.when(down(o))
        def _():
            arrived(f"gx{o}", xin.at[o])
            gout[o] = mine[o] + xin[o]
        start(f"gz{o}", gout.at[o], gin.at[o], seq(-o), down(o))

    give_near(3)
    give_near(2)

    @pl.when(down(FAR))
    def _():
        keep, give = grads(FAR)
        g4out[0] = keep
        g4out[1] = give
    start("g4", g4out, g4in, seq(-FAR), down(FAR))
    give_near(1)

    where = pl.ds(pl.multiple_of(inner * pr, pr), pr)
    arrived("b1", sin.at[1:2 * ni])
    acc = sg[0, where]
    for p, d in columns:
        acc = acc + sin[p * ni + d]
    s2[...] = acc
    for i in range(ni):
        for z in range(no):
            if i or z:
                mine_here = (inner == i) & (outer == z)
                start("b2", s2, s2in.at[i * no + z], (head, 0, 0), mine_here, False)
    sent("b2", s2, jnp.logical_not(first))

    pass_on(3)
    keep, give = grads(0)
    mine[0] = keep
    xout[0] = give
    pass_on(2)

    @pl.when(up(FAR))
    def _():
        arrived("g4", g4in)
        mine[0] += g4in[0]
        xout[0] += g4in[1]
    start("gx0", xout.at[0], xin.at[0], across)
    pass_on(1)

    def dq_part(i):
        hi = ds[i, 0]
        return dot(ktcat[i], jnp.concatenate([hi, hi, ds[i, 1]], 0), NN)

    dqt[...] = dq_part(0)
    for i in range(1, STEPS + 1):
        @pl.when(b >= (i if i < STEPS else 1))
        def _():
            dqt[...] += dq_part(i)
    dq_ref[...] = dqt[...].T

    arrived("gx0", xin.at[0])
    dkv_ref[...] = mine[0] + xin[0]
    for o in range(FAR - 1, 0, -1):
        @pl.when(up(o))
        def _():
            arrived(f"gz{o}", gin.at[o])
            dkv_ref[...] += gin[o]

    @pl.when(first)
    def _():
        arrived("b2", s2in.at[1:ni * no])
        for i in range(ni):
            part = s2in[i * no] if i else s2[...]
            for z in range(1, no):
                part = part + s2in[i * no + z]
            dkv_ref[i * pr:(i + 1) * pr] += part

    for cond, c in pending:
        when(cond, c.wait_send)
    assert len(slots) <= send.shape[0], len(slots)


def store(dq_ref, dkv_ref, dq_hbm, dk_hbm, dv_hbm, sem):
    half = dk_hbm.shape[0]
    moves = [
        (dq_ref, dq_hbm), (dkv_ref.at[0:half], dk_hbm), (dkv_ref.at[half:2 * half], dv_hbm),
    ]
    copies = [pltpu.make_async_copy(x, y, sem.at[i]) for i, (x, y) in enumerate(moves)]
    for c in copies:
        c.start()
    for c in copies:
        c.wait()


def shards(ni, no, queries, key_rows, values, out_grad, sink_len, window_len, block_codes):
    block, heads_dev, dim = queries.shape
    rows = block * heads_dev
    half = key_rows.shape[1]
    codes = block_codes.T
    pr = block // ni
    total = STEPS + 1
    sems = 23
    vmem, hbm = pl.BlockSpec(memory_space=pltpu.VMEM), pl.BlockSpec(memory_space=pltpu.HBM)
    tile = (block, dim)
    grad_q, grad_kv = pl.pallas_call(
        functools.partial(kernel, (ni, no, heads_dev)),
        out_shape=(
            pltpu.VMEM((rows, dim), f32),
            pltpu.VMEM((2 * half, block), f32),
        ),
        in_specs=[hbm] * 7,
        out_specs=(vmem,) * 2,
        scratch_shapes=[
            pltpu.SMEM(sink_len.shape, jnp.int32),
            pltpu.SMEM(window_len.shape, jnp.int32),
            pltpu.SMEM(codes.shape, jnp.int32),
            pltpu.VMEM((rows, dim), f32),
            pltpu.VMEM((rows, dim), f32),
            pltpu.SemaphoreType.DMA((7,)),
            pltpu.VMEM((STEPS, 2) + tile, f32),
            pltpu.VMEM((ni, 2, pr, dim), f32),
            pltpu.VMEM((2, pr, dim), f32),
            pltpu.VMEM((rows, 2 * dim), bf16),
            pltpu.VMEM((rows, 2 * dim), bf16),
            pltpu.VMEM((total, block, rows), f32),
            pltpu.VMEM((total, block, rows), f32),
            pltpu.VMEM((8, rows), f32),
            pltpu.VMEM((8, rows), f32),
            pltpu.VMEM((total, 2, block, rows), bf16),
            pltpu.VMEM((total, dim, 3 * block), bf16),
            pltpu.VMEM((FAR,) + tile, f32),
            pltpu.VMEM((FAR,) + tile, f32),
            pltpu.VMEM((FAR,) + tile, f32),
            pltpu.VMEM((FAR,) + tile, f32),
            pltpu.VMEM((FAR,) + tile, f32),
            pltpu.VMEM((2,) + tile, f32),
            pltpu.VMEM((2,) + tile, f32),
            pltpu.VMEM((2,) + tile, f32),
            pltpu.VMEM((2 * ni, pr, dim), f32),
            pltpu.VMEM((pr, dim), f32),
            pltpu.VMEM((ni * no, pr, dim), f32),
            pltpu.VMEM((dim, rows), f32),
            pltpu.SemaphoreType.DMA((sems,)),
            pltpu.SemaphoreType.DMA((sems,)),
        ],
        compiler_params=pltpu.CompilerParams(
            collective_id=0, has_side_effects=True, vmem_limit_bytes=66_000_000
        ),
    )(
        sink_len, window_len, codes,
        queries.reshape(rows, dim), key_rows.T, values.T, out_grad.reshape(rows, dim),
    )
    grad_q, grad_k, grad_v = pl.pallas_call(
        store,
        out_shape=(
            jax.ShapeDtypeStruct((rows, dim), f32),
            jax.ShapeDtypeStruct((half, block), f32),
            jax.ShapeDtypeStruct((half, block), f32),
        ),
        in_specs=[vmem] * 2,
        out_specs=(hbm,) * 3,
        scratch_shapes=[pltpu.SemaphoreType.DMA((3,))],
        compiler_params=pltpu.CompilerParams(vmem_limit_bytes=1 << 20),
    )(grad_q, grad_kv)
    return grad_q.reshape(queries.shape), grad_k.T, grad_v.T


def solution(mesh):
    in_specs = (
        P(("inner", "outer"), "head", None),
        P(("inner", "outer"), "head"),
        P(("inner", "outer"), "head"),
        P(("inner", "outer"), "head", None),
        P(),
        P(),
        P(),
    )
    out_specs = (
        P(("inner", "outer"), "head", None),
        P(("inner", "outer"), "head"),
        P(("inner", "outer"), "head"),
    )
    body = functools.partial(shards, mesh.shape["inner"], mesh.shape["outer"])
    return jax.shard_map(body, mesh=mesh, in_specs=in_specs, out_specs=out_specs, check_vma=False)
```

```python
import functools
import math

import jax
import jax.numpy as jnp
from jax import lax
from jax.experimental import pallas as pl
from jax.experimental.pallas import tpu as pltpu
from jax.sharding import PartitionSpec as P

STEPS = 5
FAR = STEPS - 1
DIRECT = FAR - 1
LATE = (2, 3)
BIG = 1 << 28
very_low = -1e30
f32, bf16 = jnp.float32, jnp.bfloat16
MESH = pl.DeviceIdType.MESH
NT = (((1,), (1,)), ((), ()))
NN = (((1,), (0,)), ((), ()))


def dot(a, b, dims):
    return lax.dot_general(a, b, dims, preferred_element_type=f32)


def two(x):
    hi = x.astype(bf16)
    return hi, (x - hi.astype(f32)).astype(bf16)


def when(cond, f):
    if cond is None:
        f()
    else:
        pl.when(cond)(f)


def kernel(
    sizes, sink_hbm, window_hbm, codes_hbm, q_hbm, k_hbm, v_hbm, g_hbm, dq_ref, dkv_ref,
    sink_ref, window_ref, codes_ref, q_ref, g_ref, load, buf, sinkb, piece, qcat, gcat,
    st, dp, peak, run, ds, ktcat, xout, xin, mine, gout, gin, g4out, g4in, sg, sin, s2, s2in,
    dqt, g3out, g3in, send, recv, late,
):
    ni, no, heads_dev = sizes
    half, block = k_hbm.shape
    rows = q_ref.shape[0]
    temper = 1.0 / math.sqrt(2 * half)
    head, inner, outer = lax.axis_index("head"), lax.axis_index("inner"), lax.axis_index("outer")
    par = lax.rem(head, 2)
    other = 1 - par
    partner = head + 1 - 2 * par
    count = ni * no
    b = inner * no + outer
    pr = block // ni

    def seq(o):
        t = lax.rem(b + o + count, count)
        return (head, t // no, lax.rem(t, no))

    across = (partner, inner, outer)
    columns = [(p, d) for p in range(2) for d in range(ni) if p or d]
    first = (inner == 0) & (outer == 0)
    top = outer == 0

    def column(p, d):
        return (partner if p else head, lax.rem(inner + d, ni), outer)

    def up(o):
        return b + o < count

    def down(o):
        return b >= o

    slots = {}

    def sem(name):
        return slots.setdefault(name, len(slots))

    pending = []

    def copy(name, src, dst, device):
        return pltpu.make_async_remote_copy(
            src_ref=src, dst_ref=dst, send_sem=send.at[sem(name)], recv_sem=recv.at[sem(name)],
            device_id=device, device_id_type=MESH,
        )

    def start(name, src, dst, device, cond=None, sent=True):
        c = copy(name, src, dst, device)
        when(cond, c.start)
        if sent:
            pending.append((cond, c))

    def sent(name, like, cond=None):
        pending.append((cond, copy(name, like, like, across)))

    def arrived(name, dst):
        copy(name, dst, dst, across).wait_recv()

    moves = [
        (k_hbm, buf.at[0, par, 0:half]), (v_hbm, buf.at[0, par, half:2 * half]),
        (q_hbm, q_ref), (g_hbm, g_ref),
        (codes_hbm, codes_ref), (sink_hbm, sink_ref), (window_hbm, window_ref),
    ]
    loads = [pltpu.make_async_copy(x, y, load.at[i]) for i, (x, y) in enumerate(moves)]

    barrier = pltpu.get_barrier_semaphore()

    def signal(where, device):
        pl.semaphore_signal(where, inc=1, device_id=device, device_id_type=MESH)

    def late_up(o):
        return outer + o < no

    def late_down(o):
        return outer >= o

    def one(cond, n=1):
        return jnp.where(cond, n, 0)

    def both(o):
        head_o, inner_o, outer_o = seq(o)
        return [(head, inner_o, outer_o), (partner, inner_o, outer_o)]

    signal(barrier, across)
    for d in range(1, ni):
        signal(barrier, column(0, d))
    when(top & (inner != 0), lambda: signal(barrier, (partner, 0, 0)))
    expect = ni + one(first, ni - 1)
    for o in range(1, STEPS):
        early = down(o)
        soon = up(o)
        if o in LATE:
            early = early & jnp.logical_not(late_down(o))
            soon = soon & jnp.logical_not(late_up(o))

            @pl.when(late_up(o))
            def _():
                for device in both(o)[:1 + (o == DIRECT)]:
                    signal(barrier, device)
            expect = expect + one(late_down(o), 1 + (o == DIRECT))

        @pl.when(early)
        def _():
            for device in both(-o)[:1 + (o == DIRECT)]:
                signal(barrier, device)
        expect = expect + one(soon, 1 + (o == DIRECT))

    for x in loads:
        x.start()
    pl.semaphore_wait(barrier, expect)
    for o in LATE:
        @pl.when(late_down(o))
        def _():
            for device in both(-o)[:1 + (o == DIRECT)]:
                signal(late.at[o], device)

    def entered(o):
        @pl.when(late_up(o))
        def _():
            pl.semaphore_wait(late.at[o], 1 + (o == DIRECT))

    def own_to(name, dst, devices, cond=None):
        for device in devices:
            start(name, k_hbm, dst.at[0:half], device, cond, False)
            start(name, v_hbm, dst.at[half:2 * half], device, cond, False)

    def rows_of(i):
        return (k_hbm.at[pl.ds(i * pr, pr)] if i * pr < half
                else v_hbm.at[pl.ds(i * pr - half, pr)])

    for i in range(ni):
        for p in range(2):
            if i or p:
                to = (partner if p else head, i, 0)
                start(f"f1_{p}", rows_of(i), piece.at[par], to, first, False)
    sent("f1_0", buf.at[0, 0, 0:(ni - 1) * pr], first)
    sent("f1_1", buf.at[0, 0], first)

    own_to("x0", buf.at[0, par], [across])
    sent("x0", buf.at[0, 0])
    for o in (1, FAR):
        own_to(f"w{o}", buf.at[o, par], [seq(o)], up(o))
        sent(f"w{o}", buf.at[0, 0], up(o))

    loads[2].wait()
    q0, q1 = two(q_ref[...])
    qcat[...] = jnp.concatenate([q0, q1], 1)
    loads[3].wait()
    g0, g1 = two(g_ref[...])
    gcat[...] = jnp.concatenate([g0, g1], 1)
    for i in (0, 1, 4, 5, 6):
        loads[i].wait()

    @pl.when(first)
    def _():
        piece[par] = buf[0, par, 0:pr, :]

    jk = lax.broadcasted_iota(jnp.int32, (block, rows), 0)
    iq = lax.broadcasted_iota(jnp.int32, (block, rows), 1) // heads_dev
    gap = iq - jk
    sink_end, window = sink_ref[0], window_ref[0]

    def mask_of(o):
        code = codes_ref[o, b]
        limit = jnp.where(code == 2, BIG, jnp.where(code == 1, window, -BIG)) - o * block
        here = jnp.where(b == o, sink_end, 0)
        if o == 0:
            return (gap >= 0) & ((gap < limit) | (jk < here))
        return (gap < limit) & (jk >= here)

    def scores_of(keys, vals, index, allowed):
        k0, k1 = two(keys.T)
        v0, v1 = two(vals.T)
        kk = jnp.concatenate([jnp.concatenate([k0, k0], 1), jnp.concatenate([k1, k1], 1)], 0)
        vv = jnp.concatenate([jnp.concatenate([v0, v0], 1), jnp.concatenate([v1, v1], 1)], 0)
        s = dot(kk, qcat[...], NT)
        s = jnp.where(allowed, temper * (s[0:block] + s[block:]), very_low)
        d = dot(vv, gcat[...], NT)
        d = d[0:block] + d[block:]
        t0, t1 = two(keys * temper)
        ktcat[index] = jnp.concatenate([t0, t1, t0], 1)
        high = jnp.max(s, axis=0, keepdims=True)
        if index:
            before = run[0:1]
            high = jnp.maximum(high, before)
            shrink = jnp.exp(before - high)
        e = jnp.exp(s - high)
        st[index] = e
        dp[index] = d
        norm = jnp.sum(e, axis=0, keepdims=True)
        delta = jnp.sum(e * d, axis=0, keepdims=True)
        if index:
            norm = norm + shrink * run[1:2]
            delta = delta + shrink * run[2:3]
        peak[index:index + 1] = high
        run[0:1] = high
        run[1:2] = norm
        run[2:3] = delta

    def slot(o):
        def _():
            a, c = buf[o, 0], buf[o, 1]
            scores_of(
                jnp.concatenate([a[0:half], c[0:half]], 0),
                jnp.concatenate([a[half:], c[half:]], 0), o, mask_of(o),
            )
        return _

    entered(2)
    own_to("w2", buf.at[2, par], [seq(2)], up(2))
    sent("w2", buf.at[0, 0], up(2))

    @pl.when(top)
    def _():
        @pl.when(jnp.logical_not(first))
        def _():
            arrived("f1_0", piece.at[par])
        arrived("f1_1", piece.at[other])
    start("f2", piece, piece, (head, inner, 1), top, False)
    entered(DIRECT)
    for z in range(2, no):
        start("f2", piece, piece, (head, inner, z), top, False)
    sent("f2", sinkb.at[0:no - 1], top)
    own_to(f"w{DIRECT}", buf.at[DIRECT, par], both(DIRECT), up(DIRECT))
    sent(f"w{DIRECT}", buf.at[0], up(DIRECT))

    arrived("x0", buf.at[0, other])
    start("w4x", buf.at[0, other], buf.at[FAR, other], seq(FAR), up(FAR))

    def spread():
        for d in range(1, ni):
            start("f3", piece, sinkb.at[inner], column(0, d), None, False)
        sinkb[inner] = piece[...]
    sent("f3", sinkb.at[0:ni - 1])

    def relay(o):
        @pl.when(down(o))
        def _():
            arrived(f"w{o}", buf.at[o, par])
            copy(f"r{o}", buf.at[o, par], buf.at[o, par], across).start()

    slot(0)()

    @pl.when(top)
    def _():
        spread()
        relay(2)
        relay(1)

    @pl.when(outer != 0)
    def _():
        relay(1)
        relay(2)
        arrived("f2", piece)
        spread()
    for o in (1, 2):
        pending.append((down(o), copy(f"r{o}", buf.at[o, par], buf.at[o, par], across)))

    @pl.when(down(FAR))
    def _():
        arrived(f"w{FAR}", buf.at[FAR, par])
        arrived("w4x", buf.at[FAR, other])
        slot(FAR)()

    @pl.when(down(DIRECT))
    def _():
        arrived(f"w{DIRECT}", buf.at[DIRECT])
        slot(DIRECT)()

    def last(o):
        @pl.when(down(o))
        def _():
            arrived(f"r{o}", buf.at[o, other])
            slot(o)()

    last(1)
    arrived("f3", sinkb.at[0:ni - 1])

    @pl.when(b >= 1)
    def _():
        a = [sinkb[i, p] for p in range(2) for i in range(ni)]
        cut = ni // 2
        keys = jnp.concatenate(a[0:cut] + a[ni:ni + cut], 0)
        vals = jnp.concatenate(a[cut:ni] + a[ni + cut:], 0)
        scores_of(keys, vals, STEPS, jk < sink_end)

    last(2)

    high = run[0:1]
    scale = 1.0 / run[1:2]
    delta = run[2:3] * scale

    def grads(i):
        probs = st[i] * (jnp.exp(peak[i:i + 1] - high) * scale)
        score = probs * (dp[i] - delta)
        p_hi, p_lo = two(probs)
        d_hi, d_lo = two(score)
        ds[i, 0] = d_hi
        ds[i, 1] = d_lo
        w = 2 * half
        pv = dot(jnp.concatenate([p_hi, p_lo], 0), gcat[...], NN)
        dv = pv[0:block, 0:w] + pv[0:block, w:] + pv[block:, 0:w]
        kq = dot(jnp.concatenate([d_hi, d_lo], 0), qcat[...], NN)
        dk = temper * (kq[0:block, 0:w] + kq[0:block, w:] + kq[block:, 0:w])
        dk, dv = dk.T, dv.T
        even = jnp.concatenate([dk[0:half], dv[0:half]], 0)
        odd = jnp.concatenate([dk[half:], dv[half:]], 0)
        keep = jnp.where(par == 0, even, odd)
        give = jnp.where(par == 0, odd, even)
        return keep, give

    @pl.when(b >= 1)
    def _():
        keep, give = grads(STEPS)
        sg[0] = keep
        sg[1] = give

    @pl.when(b == 0)
    def _():
        sg[...] = jnp.zeros_like(sg)

    for p, d in columns:
        target = lax.rem(inner + d, ni)
        rng = pl.ds(pl.multiple_of(target * pr, pr), pr)
        start("b1", sg.at[p, rng], sin.at[p * ni + d], column(p, d), None, False)
    sent("b1", sin.at[1:2 * ni])

    def give_near(o):
        @pl.when(down(o))
        def _():
            keep, give = grads(o)
            mine[o] = keep
            xout[o] = give
        start(f"gx{o}", xout.at[o], xin.at[o], across, down(o))

    def pass_on(o):
        @pl.when(down(o))
        def _():
            arrived(f"gx{o}", xin.at[o])
            gout[o] = mine[o] + xin[o]
        start(f"gz{o}", gout.at[o], gin.at[o], seq(-o), down(o))

    @pl.when(down(DIRECT))
    def _():
        keep, give = grads(DIRECT)
        g3out[0] = keep
        g3out[1] = give
    for p, device in enumerate(both(-DIRECT)):
        start("g3", g3out.at[p], g3in.at[p], device, down(DIRECT), False)
    sent("g3", g3out, down(DIRECT))

    give_near(2)
    give_near(1)

    @pl.when(down(FAR))
    def _():
        keep, give = grads(FAR)
        g4out[0] = keep
        g4out[1] = give
    start("g4", g4out, g4in, seq(-FAR), down(FAR))

    keep, give = grads(0)
    mine[0] = keep
    xout[0] = give

    where = pl.ds(pl.multiple_of(inner * pr, pr), pr)
    arrived("b1", sin.at[1:2 * ni])
    acc = sg[0, where]
    for p, d in columns:
        acc = acc + sin[p * ni + d]
    s2[...] = acc
    for i in range(ni):
        for z in range(no):
            if i or z:
                mine_here = (inner == i) & (outer == z)
                start("b2", s2, s2in.at[i * no + z], (head, 0, 0), mine_here, False)
    sent("b2", s2, jnp.logical_not(first))

    pass_on(2)

    @pl.when(up(FAR))
    def _():
        arrived("g4", g4in)
        mine[0] += g4in[0]
        xout[0] += g4in[1]
    start("gx0", xout.at[0], xin.at[0], across)
    pass_on(1)

    def dq_part(i):
        hi = ds[i, 0]
        return dot(ktcat[i], jnp.concatenate([hi, hi, ds[i, 1]], 0), NN)

    dqt[...] = dq_part(0)
    for i in range(1, STEPS + 1):
        @pl.when(b >= (i if i < STEPS else 1))
        def _():
            dqt[...] += dq_part(i)
    dq_ref[...] = dqt[...].T

    arrived("gx0", xin.at[0])
    dkv_ref[...] = mine[0] + xin[0]

    @pl.when(up(DIRECT))
    def _():
        arrived("g3", g3in)
        dkv_ref[...] += g3in[0] + g3in[1]
    for o in (2, 1):
        @pl.when(up(o))
        def _():
            arrived(f"gz{o}", gin.at[o])
            dkv_ref[...] += gin[o]

    @pl.when(first)
    def _():
        arrived("b2", s2in.at[1:ni * no])
        for i in range(ni):
            part = s2in[i * no] if i else s2[...]
            for z in range(1, no):
                part = part + s2in[i * no + z]
            dkv_ref[i * pr:(i + 1) * pr] += part

    for cond, c in pending:
        when(cond, c.wait_send)
    assert len(slots) <= send.shape[0], len(slots)


def store(dq_ref, dkv_ref, dq_hbm, dk_hbm, dv_hbm, sem):
    half = dk_hbm.shape[0]
    moves = [
        (dq_ref, dq_hbm), (dkv_ref.at[0:half], dk_hbm), (dkv_ref.at[half:2 * half], dv_hbm),
    ]
    copies = [pltpu.make_async_copy(x, y, sem.at[i]) for i, (x, y) in enumerate(moves)]
    for c in copies:
        c.start()
    for c in copies:
        c.wait()


def shards(ni, no, queries, key_rows, values, out_grad, sink_len, window_len, block_codes):
    block, heads_dev, dim = queries.shape
    rows = block * heads_dev
    half = key_rows.shape[1]
    codes = block_codes.T
    pr = block // ni
    total = STEPS + 1
    sems = 21
    vmem, hbm = pl.BlockSpec(memory_space=pltpu.VMEM), pl.BlockSpec(memory_space=pltpu.HBM)
    tile = (block, dim)
    grad_q, grad_kv = pl.pallas_call(
        functools.partial(kernel, (ni, no, heads_dev)),
        out_shape=(
            pltpu.VMEM((rows, dim), f32),
            pltpu.VMEM((2 * half, block), f32),
        ),
        in_specs=[hbm] * 7,
        out_specs=(vmem,) * 2,
        scratch_shapes=[
            pltpu.SMEM(sink_len.shape, jnp.int32),
            pltpu.SMEM(window_len.shape, jnp.int32),
            pltpu.SMEM(codes.shape, jnp.int32),
            pltpu.VMEM((rows, dim), f32),
            pltpu.VMEM((rows, dim), f32),
            pltpu.SemaphoreType.DMA((7,)),
            pltpu.VMEM((STEPS, 2) + tile, f32),
            pltpu.VMEM((ni, 2, pr, dim), f32),
            pltpu.VMEM((2, pr, dim), f32),
            pltpu.VMEM((rows, 2 * dim), bf16),
            pltpu.VMEM((rows, 2 * dim), bf16),
            pltpu.VMEM((total, block, rows), f32),
            pltpu.VMEM((total, block, rows), f32),
            pltpu.VMEM((8, rows), f32),
            pltpu.VMEM((8, rows), f32),
            pltpu.VMEM((total, 2, block, rows), bf16),
            pltpu.VMEM((total, dim, 3 * block), bf16),
            pltpu.VMEM((DIRECT,) + tile, f32),
            pltpu.VMEM((DIRECT,) + tile, f32),
            pltpu.VMEM((DIRECT,) + tile, f32),
            pltpu.VMEM((DIRECT,) + tile, f32),
            pltpu.VMEM((DIRECT,) + tile, f32),
            pltpu.VMEM((2,) + tile, f32),
            pltpu.VMEM((2,) + tile, f32),
            pltpu.VMEM((2,) + tile, f32),
            pltpu.VMEM((2 * ni, pr, dim), f32),
            pltpu.VMEM((pr, dim), f32),
            pltpu.VMEM((ni * no, pr, dim), f32),
            pltpu.VMEM((dim, rows), f32),
            pltpu.VMEM((2,) + tile, f32),
            pltpu.VMEM((2,) + tile, f32),
            pltpu.SemaphoreType.DMA((sems,)),
            pltpu.SemaphoreType.DMA((sems,)),
            pltpu.SemaphoreType.REGULAR((FAR,)),
        ],
        compiler_params=pltpu.CompilerParams(
            collective_id=0, has_side_effects=True, vmem_limit_bytes=66_000_000
        ),
    )(
        sink_len, window_len, codes,
        queries.reshape(rows, dim), key_rows.T, values.T, out_grad.reshape(rows, dim),
    )
    grad_q, grad_k, grad_v = pl.pallas_call(
        store,
        out_shape=(
            jax.ShapeDtypeStruct((rows, dim), f32),
            jax.ShapeDtypeStruct((half, block), f32),
            jax.ShapeDtypeStruct((half, block), f32),
        ),
        in_specs=[vmem] * 2,
        out_specs=(hbm,) * 3,
        scratch_shapes=[pltpu.SemaphoreType.DMA((3,))],
        compiler_params=pltpu.CompilerParams(vmem_limit_bytes=1 << 20),
    )(grad_q, grad_kv)
    return grad_q.reshape(queries.shape), grad_k.T, grad_v.T


def solution(mesh):
    in_specs = (
        P(("inner", "outer"), "head", None),
        P(("inner", "outer"), "head"),
        P(("inner", "outer"), "head"),
        P(("inner", "outer"), "head", None),
        P(),
        P(),
        P(),
    )
    out_specs = (
        P(("inner", "outer"), "head", None),
        P(("inner", "outer"), "head"),
        P(("inner", "outer"), "head"),
    )
    body = functools.partial(shards, mesh.shape["inner"], mesh.shape["outer"])
    return jax.shard_map(body, mesh=mesh, in_specs=in_specs, out_specs=out_specs, check_vma=False)
```

```python
import functools
import math

import jax
import jax.numpy as jnp
from jax import lax
from jax.experimental import pallas as pl
from jax.experimental.pallas import tpu as pltpu
from jax.sharding import PartitionSpec as P

STEPS = 5
FAR = STEPS - 1
DIRECT = FAR - 1
LATE = (2, 3)
ROOT = (1,)
BIG = 1 << 28
very_low = -1e30
f32, bf16 = jnp.float32, jnp.bfloat16
MESH = pl.DeviceIdType.MESH
NT = (((1,), (1,)), ((), ()))
NN = (((1,), (0,)), ((), ()))


def dot(a, b, dims):
    return lax.dot_general(a, b, dims, preferred_element_type=f32)


def two(x):
    hi = x.astype(bf16)
    return hi, (x - hi.astype(f32)).astype(bf16)


def when(cond, f):
    if cond is None:
        f()
    else:
        pl.when(cond)(f)


def kernel(
    sizes, sink_hbm, window_hbm, codes_hbm, q_hbm, k_hbm, v_hbm, g_hbm, dq_ref, dkv_ref,
    sink_ref, window_ref, codes_ref, q_ref, g_ref, load, buf, sinkb, piece, qcat, gcat,
    st, dp, peak, run, ds, ktcat, xout, xin, mine, gout, gin, g4out, g4in, sg, sin, s2, s2in,
    dqt, g3out, g3in, gdin, send, recv, late,
):
    ni, no, heads_dev = sizes
    half, block = k_hbm.shape
    rows = q_ref.shape[0]
    temper = 1.0 / math.sqrt(2 * half)
    head, inner, outer = lax.axis_index("head"), lax.axis_index("inner"), lax.axis_index("outer")
    par = lax.rem(head, 2)
    other = 1 - par
    partner = head + 1 - 2 * par
    count = ni * no
    b = inner * no + outer
    pr = block // ni

    def seq(o):
        t = lax.rem(b + o + count, count)
        return (head, t // no, lax.rem(t, no))

    across = (partner, inner, outer)
    columns = [(p, d) for p in range(2) for d in range(ni) if p or d]
    first = (inner == 0) & (outer == 0)
    top = outer == 0

    def column(p, d):
        return (partner if p else head, lax.rem(inner + d, ni), outer)

    def up(o):
        return b + o < count

    def down(o):
        return b >= o

    slots = {}

    def sem(name):
        return slots.setdefault(name, len(slots))

    pending = []

    def copy(name, src, dst, device, via=None):
        return pltpu.make_async_remote_copy(
            src_ref=src, dst_ref=dst,
            send_sem=send.at[sem(via or name)], recv_sem=recv.at[sem(name)],
            device_id=device, device_id_type=MESH,
        )

    def start(name, src, dst, device, cond=None, sent=True, via=None):
        c = copy(name, src, dst, device, via)
        when(cond, c.start)
        if sent:
            pending.append((cond, c))

    def sent(name, like, cond=None):
        pending.append((cond, copy(name, like, like, across)))

    def arrived(name, dst):
        copy(name, dst, dst, across).wait_recv()

    moves = [
        (k_hbm, buf.at[0, par, 0:half]), (v_hbm, buf.at[0, par, half:2 * half]),
        (q_hbm, q_ref), (g_hbm, g_ref),
        (codes_hbm, codes_ref), (sink_hbm, sink_ref), (window_hbm, window_ref),
    ]
    loads = [pltpu.make_async_copy(x, y, load.at[i]) for i, (x, y) in enumerate(moves)]

    barrier = pltpu.get_barrier_semaphore()

    def signal(where, device):
        pl.semaphore_signal(where, inc=1, device_id=device, device_id_type=MESH)

    end = outer == no - 1

    def both(o):
        head_o, inner_o, outer_o = seq(o)
        return [(head, inner_o, outer_o), (partner, inner_o, outer_o)]

    def one(cond, n=1):
        return jnp.where(cond, n, 0)

    far = outer >= 2
    bridged = (lax.rem(inner, 2) == 0) & (inner > 0)
    bridge = far & bridged

    def sends(o):
        if o == 2:
            return up(o) & (top | ((outer + o >= no) & (lax.rem(inner, 2) == 0)))
        return up(o)

    def hears(o):
        if o == 2:
            return down(o) & ((outer == o) | ((outer < o) & (lax.rem(inner, 2) == 1)))
        return down(o)

    signal(barrier, across)
    for d in range(1, ni):
        signal(barrier, column(0, d))
    expect = ni + one(first, ni - 1)
    when(top & (inner != 0), lambda: signal(barrier, (partner, 0, 0)))
    for o in range(1, STEPS):
        asks, tells = sends(o), hears(o)
        if o in LATE:
            asks, tells = asks & (outer != 0), tells & (outer != o)
        when(tells, lambda: signal(barrier, seq(-o)))
        expect = expect + one(asks)
    for o in LATE:
        when(top, lambda: signal(barrier, seq(o)))
    near_bridge = (outer < 2) & bridged
    when(near_bridge, lambda: signal(barrier, seq(2)))
    expect = expect + one(far) + one(bridge)

    for x in loads:
        x.start()
    pl.semaphore_wait(barrier, expect)
    for i, o in enumerate(LATE):
        when(outer == o, lambda: signal(late.at[i], seq(-o)))

    def own_to(name, dst, devices, cond=None):
        for device in devices:
            start(name, k_hbm, dst.at[0:half], device, cond, False)
            start(name, v_hbm, dst.at[half:2 * half], device, cond, False)

    def rows_of(i):
        return (k_hbm.at[pl.ds(i * pr, pr)] if i * pr < half
                else v_hbm.at[pl.ds(i * pr - half, pr)])

    for i in range(ni):
        for p in range(2):
            if i or p:
                to = (partner if p else head, i, 0)
                start(f"f1_{p}", rows_of(i), piece.at[par], to, first, False)
    sent("f1_0", buf.at[0, 0, 0:(ni - 1) * pr], first)
    sent("f1_1", buf.at[0, 0], first)

    own_to("x0", buf.at[0, par], [across])
    sent("x0", buf.at[0, 0])
    for o in range(1, STEPS):
        sent(f"w{o}", buf.at[0, 0], sends(o))
        now = sends(o) & (outer != 0) if o in LATE else sends(o)
        own_to(f"w{o}", buf.at[o, par], [seq(o)], now)

    loads[2].wait()
    q0, q1 = two(q_ref[...])
    qcat[...] = jnp.concatenate([q0, q1], 1)
    loads[3].wait()
    g0, g1 = two(g_ref[...])
    gcat[...] = jnp.concatenate([g0, g1], 1)
    for i in (0, 1, 4, 5, 6):
        loads[i].wait()

    @pl.when(first)
    def _():
        piece[par] = buf[0, par, 0:pr, :]

    jk = lax.broadcasted_iota(jnp.int32, (block, rows), 0)
    iq = lax.broadcasted_iota(jnp.int32, (block, rows), 1) // heads_dev
    gap = iq - jk
    sink_end, window = sink_ref[0], window_ref[0]

    def mask_of(o):
        code = codes_ref[o, b]
        limit = jnp.where(code == 2, BIG, jnp.where(code == 1, window, -BIG)) - o * block
        here = jnp.where(b == o, sink_end, 0)
        if o == 0:
            return (gap >= 0) & ((gap < limit) | (jk < here))
        return (gap < limit) & (jk >= here)

    def scores_of(keys, vals, index, allowed):
        k0, k1 = two(keys.T)
        v0, v1 = two(vals.T)
        kk = jnp.concatenate([jnp.concatenate([k0, k0], 1), jnp.concatenate([k1, k1], 1)], 0)
        vv = jnp.concatenate([jnp.concatenate([v0, v0], 1), jnp.concatenate([v1, v1], 1)], 0)
        s = dot(kk, qcat[...], NT)
        s = jnp.where(allowed, temper * (s[0:block] + s[block:]), very_low)
        d = dot(vv, gcat[...], NT)
        d = d[0:block] + d[block:]
        t0, t1 = two(keys * temper)
        ktcat[index] = jnp.concatenate([t0, t1, t0], 1)
        high = jnp.max(s, axis=0, keepdims=True)
        if index:
            before = run[0:1]
            high = jnp.maximum(high, before)
            shrink = jnp.exp(before - high)
        e = jnp.exp(s - high)
        st[index] = e
        dp[index] = d
        norm = jnp.sum(e, axis=0, keepdims=True)
        delta = jnp.sum(e * d, axis=0, keepdims=True)
        if index:
            norm = norm + shrink * run[1:2]
            delta = delta + shrink * run[2:3]
        peak[index:index + 1] = high
        run[0:1] = high
        run[1:2] = norm
        run[2:3] = delta

    def slot(o):
        def _():
            a, c = buf[o, 0], buf[o, 1]
            scores_of(
                jnp.concatenate([a[0:half], c[0:half]], 0),
                jnp.concatenate([a[half:], c[half:]], 0), o, mask_of(o),
            )
        return _

    def relay(o):
        @pl.when(down(o))
        def _():
            arrived(f"w{o}", buf.at[o, par])
            copy(f"r{o}", buf.at[o, par], buf.at[o, par], across).start()

    @pl.when(top)
    def _():
        pl.semaphore_wait(late.at[0], 1)
        own_to("w2", buf.at[2, par], [seq(2)])

        @pl.when(jnp.logical_not(first))
        def _():
            arrived("f1_0", piece.at[par])
        arrived("f1_1", piece.at[other])
        start("f2", piece, piece, (head, inner, 1), None, False)
        pl.semaphore_wait(late.at[1], 1)
        for z in range(no - 1, 1, -1):
            start("f2", piece, piece, (head, inner, z), None, False)
        own_to("w3", buf.at[3, par], [seq(3)])
    sent("f2", sinkb.at[0:no - 1], top)

    @pl.when(outer != 0)
    def _():
        relay(1)

    between = outer == no - 2
    start("w2", buf.at[1, par], buf.at[2, par], seq(1), between, False, "on")
    pending.append((between, copy("w2", buf.at[1, par], buf.at[2, par], across, "on")))

    @pl.when(bridge)
    def _():
        arrived(f"w{FAR}", buf.at[FAR, par])
    start("w2", buf.at[FAR, par], buf.at[2, par], seq(-2), bridge, False, "over")
    pending.append((bridge, copy("w2", buf.at[FAR, par], buf.at[2, par], across, "over")))

    arrived("x0", buf.at[0, other])
    start("w3x", buf.at[0, other], buf.at[3, other], seq(3), up(3))
    start("w4x", buf.at[0, other], buf.at[FAR, other], seq(FAR), up(FAR))

    def spread():
        for d in range(1, ni):
            start("f3", piece, sinkb.at[inner], column(0, d), None, False)
        sinkb[inner] = piece[...]
    sent("f3", sinkb.at[0:ni - 1])

    def sink():
        arrived("f2", piece)
        spread()

    slot(0)()

    @pl.when(top)
    def _():
        spread()

        @pl.when(bridged)
        def _():
            relay(1)
            relay(2)

        @pl.when(jnp.logical_not(bridged))
        def _():
            relay(2)
            relay(1)

    @pl.when(outer == 1)
    def _():
        sink()
        relay(2)

    @pl.when(outer > 1)
    def _():
        relay(2)
        sink()
    for o in (1, 2):
        pending.append((down(o), copy(f"r{o}", buf.at[o, par], buf.at[o, par], across)))

    @pl.when(down(FAR))
    def _():
        @pl.when(jnp.logical_not(bridge))
        def _():
            arrived(f"w{FAR}", buf.at[FAR, par])
        arrived("w4x", buf.at[FAR, other])
        slot(FAR)()

    def last(o):
        @pl.when(down(o))
        def _():
            arrived(f"r{o}", buf.at[o, other])
            slot(o)()

    def sinks():
        arrived("f3", sinkb.at[0:ni - 1])

        @pl.when(b >= 1)
        def _():
            a = [sinkb[i, p] for p in range(2) for i in range(ni)]
            cut = ni // 2
            keys = jnp.concatenate(a[0:cut] + a[ni:ni + cut], 0)
            vals = jnp.concatenate(a[cut:ni] + a[ni + cut:], 0)
            scores_of(keys, vals, STEPS, jk < sink_end)

    def third():
        @pl.when(down(3))
        def _():
            arrived("w3", buf.at[3, par])
            arrived("w3x", buf.at[3, other])
            slot(3)()

    @pl.when(top)
    def _():
        third()
        sinks()

        @pl.when(bridged)
        def _():
            last(1)
            last(2)

        @pl.when(jnp.logical_not(bridged))
        def _():
            last(2)
            last(1)

    @pl.when((outer != 0) & jnp.logical_not(end))
    def _():
        third()
        last(1)
        last(2)
        sinks()

    @pl.when(end)
    def _():
        last(1)
        last(2)
        sinks()
        third()

    high = run[0:1]
    scale = 1.0 / run[1:2]
    delta = run[2:3] * scale

    def grads(i):
        probs = st[i] * (jnp.exp(peak[i:i + 1] - high) * scale)
        score = probs * (dp[i] - delta)
        p_hi, p_lo = two(probs)
        d_hi, d_lo = two(score)
        ds[i, 0] = d_hi
        ds[i, 1] = d_lo
        w = 2 * half
        pv = dot(jnp.concatenate([p_hi, p_lo], 0), gcat[...], NN)
        dv = pv[0:block, 0:w] + pv[0:block, w:] + pv[block:, 0:w]
        kq = dot(jnp.concatenate([d_hi, d_lo], 0), qcat[...], NN)
        dk = temper * (kq[0:block, 0:w] + kq[0:block, w:] + kq[block:, 0:w])
        dk, dv = dk.T, dv.T
        even = jnp.concatenate([dk[0:half], dv[0:half]], 0)
        odd = jnp.concatenate([dk[half:], dv[half:]], 0)
        keep = jnp.where(par == 0, even, odd)
        give = jnp.where(par == 0, odd, even)
        return keep, give

    def at_root(o):
        return b == (o if o in ROOT else -1)

    def give_near(o):
        @pl.when(down(o))
        def _():
            keep, give = grads(o)
            mine[o] = keep
            xout[o] = give
        c = copy(f"gx{o}", xout.at[o], xin.at[o], across)
        when(down(o) & (~at_root(o)), c.start)
        if o not in ROOT:
            return
        start(f"gd{o}", mine.at[o], gdin.at[o - 1, 0], (head, 0, 0), at_root(o), False)
        start(f"gd{o}", xout.at[o], gdin.at[o - 1, 1], (partner, 0, 0), at_root(o), False)
        sent(f"gd{o}", g3out, at_root(o))

    def pass_on(o):
        @pl.when(down(o) & (~at_root(o)))
        def _():
            arrived(f"gx{o}", xin.at[o])
            gout[o] = mine[o] + xin[o]
        c = copy(f"gz{o}", gout.at[o], gin.at[o], seq(-o))
        when(down(o) & (~at_root(o)), c.start)

    for o in (1, 2):
        for name in ("gx", "gz"):
            c = copy(f"{name}{o}", xout.at[o], xin.at[o], across)
            pending.append((down(o) & (~at_root(o)), c))

    @pl.when(outer == 2)
    def _():
        give_near(2)

    @pl.when(b >= 1)
    def _():
        keep, give = grads(STEPS)
        sg[0] = keep
        sg[1] = give

    @pl.when(b == 0)
    def _():
        sg[...] = jnp.zeros_like(sg)

    for p, d in columns[::-1]:
        target = lax.rem(inner + d, ni)
        rng = pl.ds(pl.multiple_of(target * pr, pr), pr)
        start("b1", sg.at[p, rng], sin.at[p * ni + d], column(p, d), None, False)
    sent("b1", sin.at[1:2 * ni])

    @pl.when(down(3))
    def _():
        keep, give = grads(3)
        g3out[0] = keep
        g3out[1] = give
    for p, device in enumerate(both(-3)):
        start("g3", g3out.at[p], g3in.at[p], device, down(3) & end if p else down(3), False)
    start("g3", g3out.at[1], g3in.at[1], seq(-3), down(3) & jnp.logical_not(end), False)
    sent("g3", g3out, down(3))

    @pl.when(outer != 2)
    def _():
        give_near(2)
    give_near(1)

    @pl.when(down(FAR))
    def _():
        keep, give = grads(FAR)
        g4out[0] = keep
        g4out[1] = give
    start("g4", g4out, g4in, seq(-FAR), down(FAR))

    keep, give = grads(0)
    mine[0] = keep
    xout[0] = give

    where = pl.ds(pl.multiple_of(inner * pr, pr), pr)
    @pl.when(outer == 2)
    def _():
        pass_on(2)
    arrived("b1", sin.at[1:2 * ni])
    acc = sg[0, where]
    for p, d in columns:
        acc = acc + sin[p * ni + d]
    s2[...] = acc
    for i in range(ni):
        for z in range(no):
            if i or z:
                mine_here = (inner == i) & (outer == z)
                start("b2", s2, s2in.at[i * no + z], (head, 0, 0), mine_here, False)
    sent("b2", s2, jnp.logical_not(first))

    @pl.when(outer != 2)
    def _():
        pass_on(2)
    pass_on(1)

    def join(cond, name, ref):
        @pl.when(cond)
        def _():
            arrived(name, ref)
            mine[0] += ref[0]
            xout[0] += ref[1]

    join(up(FAR), "g4", g4in)
    join(up(3) & jnp.logical_not(top), "g3", g3in)
    start("gx0", xout.at[0], xin.at[0], across)

    def dq_part(i):
        hi = ds[i, 0]
        return dot(ktcat[i], jnp.concatenate([hi, hi, ds[i, 1]], 0), NN)

    dqt[...] = dq_part(0)
    for i in range(1, STEPS + 1):
        @pl.when(b >= (i if i < STEPS else 1))
        def _():
            dqt[...] += dq_part(i)
    dq_ref[...] = dqt[...].T

    arrived("gx0", xin.at[0])
    dkv_ref[...] = mine[0] + xin[0]


    @pl.when(up(3) & top)
    def _():
        arrived("g3", g3in)
        dkv_ref[...] += g3in[0] + g3in[1]
    for o in ROOT:
        @pl.when(first)
        def _():
            arrived(f"gd{o}", gdin.at[o - 1])
            dkv_ref[...] += gdin[o - 1, 0] + gdin[o - 1, 1]
    for o in (2, 1):
        @pl.when(up(o) & jnp.logical_not(first) if o in ROOT else up(o))
        def _():
            arrived(f"gz{o}", gin.at[o])
            dkv_ref[...] += gin[o]

    @pl.when(first)
    def _():
        arrived("b2", s2in.at[1:ni * no])
        for i in range(ni):
            part = s2in[i * no] if i else s2[...]
            for z in range(1, no):
                part = part + s2in[i * no + z]
            dkv_ref[i * pr:(i + 1) * pr] += part

    for cond, c in pending:
        when(cond, c.wait_send)
    assert len(slots) <= send.shape[0], len(slots)


def store(dq_ref, dkv_ref, dq_hbm, dk_hbm, dv_hbm, sem):
    half = dk_hbm.shape[0]
    moves = [
        (dq_ref, dq_hbm), (dkv_ref.at[0:half], dk_hbm), (dkv_ref.at[half:2 * half], dv_hbm),
    ]
    copies = [pltpu.make_async_copy(x, y, sem.at[i]) for i, (x, y) in enumerate(moves)]
    for c in copies:
        c.start()
    for c in copies:
        c.wait()


def shards(ni, no, queries, key_rows, values, out_grad, sink_len, window_len, block_codes):
    block, heads_dev, dim = queries.shape
    rows = block * heads_dev
    half = key_rows.shape[1]
    codes = block_codes.T
    pr = block // ni
    total = STEPS + 1
    sems = 26
    vmem, hbm = pl.BlockSpec(memory_space=pltpu.VMEM), pl.BlockSpec(memory_space=pltpu.HBM)
    tile = (block, dim)
    grad_q, grad_kv = pl.pallas_call(
        functools.partial(kernel, (ni, no, heads_dev)),
        out_shape=(
            pltpu.VMEM((rows, dim), f32),
            pltpu.VMEM((2 * half, block), f32),
        ),
        in_specs=[hbm] * 7,
        out_specs=(vmem,) * 2,
        scratch_shapes=[
            pltpu.SMEM(sink_len.shape, jnp.int32),
            pltpu.SMEM(window_len.shape, jnp.int32),
            pltpu.SMEM(codes.shape, jnp.int32),
            pltpu.VMEM((rows, dim), f32),
            pltpu.VMEM((rows, dim), f32),
            pltpu.SemaphoreType.DMA((7,)),
            pltpu.VMEM((STEPS, 2) + tile, f32),
            pltpu.VMEM((ni, 2, pr, dim), f32),
            pltpu.VMEM((2, pr, dim), f32),
            pltpu.VMEM((rows, 2 * dim), bf16),
            pltpu.VMEM((rows, 2 * dim), bf16),
            pltpu.VMEM((total, block, rows), f32),
            pltpu.VMEM((total, block, rows), f32),
            pltpu.VMEM((8, rows), f32),
            pltpu.VMEM((8, rows), f32),
            pltpu.VMEM((total, 2, block, rows), bf16),
            pltpu.VMEM((total, dim, 3 * block), bf16),
            pltpu.VMEM((DIRECT,) + tile, f32),
            pltpu.VMEM((DIRECT,) + tile, f32),
            pltpu.VMEM((DIRECT,) + tile, f32),
            pltpu.VMEM((DIRECT,) + tile, f32),
            pltpu.VMEM((DIRECT,) + tile, f32),
            pltpu.VMEM((2,) + tile, f32),
            pltpu.VMEM((2,) + tile, f32),
            pltpu.VMEM((2,) + tile, f32),
            pltpu.VMEM((2 * ni, pr, dim), f32),
            pltpu.VMEM((pr, dim), f32),
            pltpu.VMEM((ni * no, pr, dim), f32),
            pltpu.VMEM((dim, rows), f32),
            pltpu.VMEM((2,) + tile, f32),
            pltpu.VMEM((2,) + tile, f32),
            pltpu.VMEM((2, 2) + tile, f32),
            pltpu.SemaphoreType.DMA((sems,)),
            pltpu.SemaphoreType.DMA((sems,)),
            pltpu.SemaphoreType.REGULAR((2,)),
        ],
        compiler_params=pltpu.CompilerParams(
            collective_id=0, has_side_effects=True, vmem_limit_bytes=66_000_000
        ),
    )(
        sink_len, window_len, codes,
        queries.reshape(rows, dim), key_rows.T, values.T, out_grad.reshape(rows, dim),
    )
    grad_q, grad_k, grad_v = pl.pallas_call(
        store,
        out_shape=(
            jax.ShapeDtypeStruct((rows, dim), f32),
            jax.ShapeDtypeStruct((half, block), f32),
            jax.ShapeDtypeStruct((half, block), f32),
        ),
        in_specs=[vmem] * 2,
        out_specs=(hbm,) * 3,
        scratch_shapes=[pltpu.SemaphoreType.DMA((3,))],
        compiler_params=pltpu.CompilerParams(vmem_limit_bytes=1 << 20),
    )(grad_q, grad_kv)
    return grad_q.reshape(queries.shape), grad_k.T, grad_v.T


def solution(mesh):
    in_specs = (
        P(("inner", "outer"), "head", None),
        P(("inner", "outer"), "head"),
        P(("inner", "outer"), "head"),
        P(("inner", "outer"), "head", None),
        P(),
        P(),
        P(),
    )
    out_specs = (
        P(("inner", "outer"), "head", None),
        P(("inner", "outer"), "head"),
        P(("inner", "outer"), "head"),
    )
    body = functools.partial(shards, mesh.shape["inner"], mesh.shape["outer"])
    return jax.shard_map(body, mesh=mesh, in_specs=in_specs, out_specs=out_specs, check_vma=False)
```

```python
import functools
import math

import jax
import jax.numpy as jnp
from jax import lax
from jax.experimental import pallas as pl
from jax.experimental.pallas import tpu as pltpu
from jax.sharding import PartitionSpec as P

STEPS = 5
FAR = STEPS - 1
DIRECT = FAR - 1
LATE = (2, 3)
ROOT = (1,)
BIG = 1 << 28
very_low = -1e30
SENT = {
    "x0": "all", "f3": "all", "b1": "all", "gx0": "all", "w3x": "w3", "w4x": "w4",
    "r1": "d1", "gx1": "d1", "gz1": "d1", "gd1": "d1", "r2": "d2", "gx2": "d2", "gz2": "d2",
    "f1_0": "f1", "f1_1": "f1",
}
CAME = {"w3x": "w3", "f1_0": "f1", "f1_1": "f1"}
f32, bf16 = jnp.float32, jnp.bfloat16
MESH = pl.DeviceIdType.MESH
NT = (((1,), (1,)), ((), ()))
NN = (((1,), (0,)), ((), ()))


def dot(a, b, dims):
    return lax.dot_general(a, b, dims, preferred_element_type=f32)


def two(x):
    hi = x.astype(bf16)
    return hi, (x - hi.astype(f32)).astype(bf16)


def when(cond, f):
    if cond is None:
        f()
    else:
        pl.when(cond)(f)


def kernel(
    sizes, sink_hbm, window_hbm, codes_hbm, q_hbm, k_hbm, v_hbm, g_hbm, dq_ref, dkv_ref,
    sink_ref, window_ref, codes_ref, q_ref, g_ref, load, buf, sinkb, piece, qcat, gcat,
    st, dp, peak, run, ds, ktcat, xout, xin, mine, gout, gin, g4out, g4in, sg, sin, s2, s2in,
    dqt, g3out, g3in, gdin, tally, send, recv, late,
):
    ni, no, heads_dev = sizes
    half, block = k_hbm.shape
    rows = q_ref.shape[0]
    temper = 1.0 / math.sqrt(2 * half)
    head, inner, outer = lax.axis_index("head"), lax.axis_index("inner"), lax.axis_index("outer")
    par = lax.rem(head, 2)
    other = 1 - par
    partner = head + 1 - 2 * par
    count = ni * no
    b = inner * no + outer
    pr = block // ni

    def seq(o):
        t = lax.rem(b + o + count, count)
        return (head, t // no, lax.rem(t, no))

    across = (partner, inner, outer)
    columns = [(p, d) for p in range(2) for d in range(ni) if p or d]
    first = (inner == 0) & (outer == 0)
    top = outer == 0

    def column(p, d):
        return (partner if p else head, lax.rem(inner + d, ni), outer)

    def up(o):
        return b + o < count

    def down(o):
        return b >= o

    sent_slots, slots = {}, {}

    def numbered(table, name):
        return table.setdefault(name, len(table))

    def copy(name, src, dst, device, via=None):
        out = numbered(sent_slots, SENT.get(via or name, via or name))
        return pltpu.make_async_remote_copy(
            src_ref=src, dst_ref=dst,
            send_sem=send.at[out], recv_sem=recv.at[numbered(slots, CAME.get(name, name))],
            device_id=device, device_id_type=MESH,
        )

    def start(name, src, dst, device, cond=None, via=None):
        when(cond, copy(name, src, dst, device, via).start)

    def arrived(name, dst):
        pltpu.make_async_remote_copy(
            src_ref=dst, dst_ref=dst, send_sem=send.at[0],
            recv_sem=recv.at[numbered(slots, CAME.get(name, name))],
            device_id=across, device_id_type=MESH,
        ).wait_recv()

    moves = [
        (k_hbm, buf.at[0, par, 0:half]), (v_hbm, buf.at[0, par, half:2 * half]),
        (q_hbm, q_ref), (g_hbm, g_ref),
        (codes_hbm, codes_ref), (sink_hbm, sink_ref), (window_hbm, window_ref),
    ]
    loads = [pltpu.make_async_copy(x, y, load.at[i]) for i, (x, y) in enumerate(moves)]

    barrier = pltpu.get_barrier_semaphore()

    def signal(where, device):
        pl.semaphore_signal(where, inc=1, device_id=device, device_id_type=MESH)

    end = outer == no - 1

    def both(o):
        head_o, inner_o, outer_o = seq(o)
        return [(head, inner_o, outer_o), (partner, inner_o, outer_o)]

    def one(cond, n=1):
        return jnp.where(cond, n, 0)

    far = outer >= 2
    bridged = (lax.rem(inner, 2) == 0) & (inner > 0)
    bridge = far & bridged

    def sends(o):
        if o == 2:
            return up(o) & (top | ((outer + o >= no) & (lax.rem(inner, 2) == 0)))
        return up(o)

    def hears(o):
        if o == 2:
            return down(o) & ((outer == o) | ((outer < o) & (lax.rem(inner, 2) == 1)))
        return down(o)

    signal(barrier, across)
    for d in range(1, ni):
        signal(barrier, column(0, d))
    expect = ni + one(first, ni - 1)
    when(top & (inner != 0), lambda: signal(barrier, (partner, 0, 0)))
    for o in range(1, STEPS):
        asks, tells = sends(o), hears(o)
        if o in LATE:
            asks, tells = asks & (outer != 0), tells & (outer != o)
        when(tells, lambda: signal(barrier, seq(-o)))
        expect = expect + one(asks)
    for o in LATE:
        when(top, lambda: signal(barrier, seq(o)))
    near_bridge = (outer < 2) & bridged
    when(near_bridge, lambda: signal(barrier, seq(2)))
    expect = expect + one(far) + one(bridge)

    for x in loads:
        x.start()
    pl.semaphore_wait(barrier, expect)
    for i, o in enumerate(LATE):
        when(outer == o, lambda: signal(late.at[i], seq(-o)))

    def own_to(name, dst, devices, cond=None):
        for device in devices:
            start(name, k_hbm, dst.at[0:half], device, cond)
            start(name, v_hbm, dst.at[half:2 * half], device, cond)

    def rows_of(i):
        return (k_hbm.at[pl.ds(i * pr, pr)] if i * pr < half
                else v_hbm.at[pl.ds(i * pr - half, pr)])

    for i in range(ni):
        for p in range(2):
            if i or p:
                to = (partner if p else head, i, 0)
                start(f"f1_{p}", rows_of(i), piece.at[par], to, first)

    own_to("x0", buf.at[0, par], [across])
    for o in range(1, STEPS):
        now = sends(o) & (outer != 0) if o in LATE else sends(o)
        own_to(f"w{o}", buf.at[o, par], [seq(o)], now)

    loads[2].wait()
    q0, q1 = two(q_ref[...])
    qcat[...] = jnp.concatenate([q0, q1], 1)
    loads[3].wait()
    g0, g1 = two(g_ref[...])
    gcat[...] = jnp.concatenate([g0, g1], 1)
    for i in (0, 1, 4, 5, 6):
        loads[i].wait()

    @pl.when(first)
    def _():
        piece[par] = buf[0, par, 0:pr, :]

    jk = lax.broadcasted_iota(jnp.int32, (block, rows), 0)
    iq = lax.broadcasted_iota(jnp.int32, (block, rows), 1) // heads_dev
    gap = iq - jk
    sink_end, window = sink_ref[0], window_ref[0]

    def mask_of(o):
        code = codes_ref[o, b]
        limit = jnp.where(code == 2, BIG, jnp.where(code == 1, window, -BIG)) - o * block
        here = jnp.where(b == o, sink_end, 0)
        if o == 0:
            return (gap >= 0) & ((gap < limit) | (jk < here))
        return (gap < limit) & (jk >= here)

    def scores_of(keys, vals, index, allowed):
        k0, k1 = two(keys.T)
        v0, v1 = two(vals.T)
        kk = jnp.concatenate([jnp.concatenate([k0, k0], 1), jnp.concatenate([k1, k1], 1)], 0)
        vv = jnp.concatenate([jnp.concatenate([v0, v0], 1), jnp.concatenate([v1, v1], 1)], 0)
        s = dot(kk, qcat[...], NT)
        s = jnp.where(allowed, temper * (s[0:block] + s[block:]), very_low)
        d = dot(vv, gcat[...], NT)
        d = d[0:block] + d[block:]
        t0, t1 = two(keys * temper)
        ktcat[index] = jnp.concatenate([t0, t1, t0], 1)
        high = jnp.max(s, axis=0, keepdims=True)
        if index:
            before = run[0:1]
            high = jnp.maximum(high, before)
            shrink = jnp.exp(before - high)
        e = jnp.exp(s - high)
        st[index] = e
        dp[index] = d
        norm = jnp.sum(e, axis=0, keepdims=True)
        delta = jnp.sum(e * d, axis=0, keepdims=True)
        if index:
            norm = norm + shrink * run[1:2]
            delta = delta + shrink * run[2:3]
        peak[index:index + 1] = high
        run[0:1] = high
        run[1:2] = norm
        run[2:3] = delta

    def slot(o):
        def _():
            a, c = buf[o, 0], buf[o, 1]
            scores_of(
                jnp.concatenate([a[0:half], c[0:half]], 0),
                jnp.concatenate([a[half:], c[half:]], 0), o, mask_of(o),
            )
        return _

    def relay(o):
        @pl.when(down(o))
        def _():
            arrived(f"w{o}", buf.at[o, par])
            copy(f"r{o}", buf.at[o, par], buf.at[o, par], across).start()

    @pl.when(top)
    def _():
        pl.semaphore_wait(late.at[0], 1)
        own_to("w2", buf.at[2, par], [seq(2)])

        @pl.when(jnp.logical_not(first))
        def _():
            arrived("f1", piece)

        @pl.when(first)
        def _():
            arrived("f1", piece.at[other])
        start("f2", piece, piece, (head, inner, 1))
        pl.semaphore_wait(late.at[1], 1)
        for z in range(no - 1, 1, -1):
            start("f2", piece, piece, (head, inner, z))
        own_to("w3", buf.at[3, par], [seq(3)])

    @pl.when(outer != 0)
    def _():
        relay(1)

    between = outer == no - 2
    start("w2", buf.at[1, par], buf.at[2, par], seq(1), between, "on")

    @pl.when(bridge)
    def _():
        arrived(f"w{FAR}", buf.at[FAR, par])
    start("w2", buf.at[FAR, par], buf.at[2, par], seq(-2), bridge, "over")

    arrived("x0", buf.at[0, other])
    start("w3x", buf.at[0, other], buf.at[3, other], seq(3), up(3))
    start("w4x", buf.at[0, other], buf.at[FAR, other], seq(FAR), up(FAR))

    def spread():
        for d in range(1, ni):
            start("f3", piece, sinkb.at[inner], column(0, d))
        sinkb[inner] = piece[...]

    def sink():
        arrived("f2", piece)
        spread()

    slot(0)()

    @pl.when(top)
    def _():
        spread()

        @pl.when(bridged)
        def _():
            relay(1)
            relay(2)

        @pl.when(jnp.logical_not(bridged))
        def _():
            relay(2)
            relay(1)

    @pl.when(outer == 1)
    def _():
        sink()
        relay(2)

    @pl.when(outer > 1)
    def _():
        relay(2)
        sink()

    @pl.when(down(FAR))
    def _():
        @pl.when(jnp.logical_not(bridge))
        def _():
            arrived(f"w{FAR}", buf.at[FAR, par])
        arrived("w4x", buf.at[FAR, other])
        slot(FAR)()

    def last(o):
        @pl.when(down(o))
        def _():
            arrived(f"r{o}", buf.at[o, other])
            slot(o)()

    def sinks():
        arrived("f3", sinkb.at[0:ni - 1])

        @pl.when(b >= 1)
        def _():
            a = [sinkb[i, p] for p in range(2) for i in range(ni)]
            cut = ni // 2
            keys = jnp.concatenate(a[0:cut] + a[ni:ni + cut], 0)
            vals = jnp.concatenate(a[cut:ni] + a[ni + cut:], 0)
            scores_of(keys, vals, STEPS, jk < sink_end)

    def third():
        @pl.when(down(3))
        def _():
            arrived("w3", buf.at[3])
            slot(3)()

    @pl.when(top)
    def _():
        third()
        sinks()

        @pl.when(bridged)
        def _():
            last(1)
            last(2)

        @pl.when(jnp.logical_not(bridged))
        def _():
            last(2)
            last(1)

    @pl.when((outer != 0) & jnp.logical_not(end))
    def _():
        third()
        last(1)
        last(2)
        sinks()

    @pl.when(end)
    def _():
        last(1)
        last(2)
        sinks()
        third()

    high = run[0:1]
    scale = 1.0 / run[1:2]
    delta = run[2:3] * scale

    def grads(i):
        probs = st[i] * (jnp.exp(peak[i:i + 1] - high) * scale)
        score = probs * (dp[i] - delta)
        p_hi, p_lo = two(probs)
        d_hi, d_lo = two(score)
        ds[i, 0] = d_hi
        ds[i, 1] = d_lo
        w = 2 * half
        pv = dot(jnp.concatenate([p_hi, p_lo], 0), gcat[...], NN)
        dv = pv[0:block, 0:w] + pv[0:block, w:] + pv[block:, 0:w]
        kq = dot(jnp.concatenate([d_hi, d_lo], 0), qcat[...], NN)
        dk = temper * (kq[0:block, 0:w] + kq[0:block, w:] + kq[block:, 0:w])
        dk, dv = dk.T, dv.T
        even = jnp.concatenate([dk[0:half], dv[0:half]], 0)
        odd = jnp.concatenate([dk[half:], dv[half:]], 0)
        keep = jnp.where(par == 0, even, odd)
        give = jnp.where(par == 0, odd, even)
        return keep, give

    def at_root(o):
        return b == (o if o in ROOT else -1)

    def give_near(o):
        @pl.when(down(o))
        def _():
            keep, give = grads(o)
            mine[o] = keep
            xout[o] = give
        c = copy(f"gx{o}", xout.at[o], xin.at[o], across)
        when(down(o) & (~at_root(o)), c.start)
        if o not in ROOT:
            return
        start(f"gd{o}", mine.at[o], gdin.at[o - 1, 0], (head, 0, 0), at_root(o))
        start(f"gd{o}", xout.at[o], gdin.at[o - 1, 1], (partner, 0, 0), at_root(o))

    def pass_on(o):
        @pl.when(down(o) & (~at_root(o)))
        def _():
            arrived(f"gx{o}", xin.at[o])
            gout[o] = mine[o] + xin[o]
        c = copy(f"gz{o}", gout.at[o], gin.at[o], seq(-o))
        when(down(o) & (~at_root(o)), c.start)

    @pl.when(outer == 2)
    def _():
        give_near(2)

    @pl.when(b >= 1)
    def _():
        keep, give = grads(STEPS)
        sg[0] = keep
        sg[1] = give

    @pl.when(b == 0)
    def _():
        sg[...] = jnp.zeros_like(sg)

    for p, d in columns[::-1]:
        target = lax.rem(inner + d, ni)
        rng = pl.ds(pl.multiple_of(target * pr, pr), pr)
        start("b1", sg.at[p, rng], sin.at[p * ni + d], column(p, d))

    @pl.when(down(3))
    def _():
        keep, give = grads(3)
        g3out[0] = keep
        g3out[1] = give
    for p, device in enumerate(both(-3)):
        start("g3", g3out.at[p], g3in.at[p], device, down(3) & end if p else down(3))
    start("g3", g3out.at[1], g3in.at[1], seq(-3), down(3) & jnp.logical_not(end))

    @pl.when(outer != 2)
    def _():
        give_near(2)
    give_near(1)

    @pl.when(down(FAR))
    def _():
        keep, give = grads(FAR)
        g4out[0] = keep
        g4out[1] = give
    start("g4", g4out, g4in, seq(-FAR), down(FAR))

    keep, give = grads(0)
    mine[0] = keep
    xout[0] = give

    where = pl.ds(pl.multiple_of(inner * pr, pr), pr)
    @pl.when(outer == 2)
    def _():
        pass_on(2)
    arrived("b1", sin.at[1:2 * ni])
    acc = sg[0, where]
    for p, d in columns:
        acc = acc + sin[p * ni + d]
    s2[...] = acc
    for i in range(ni):
        for z in range(no):
            if i or z:
                mine_here = (inner == i) & (outer == z)
                start("b2", s2, s2in.at[i * no + z], (head, 0, 0), mine_here)

    @pl.when(outer != 2)
    def _():
        pass_on(2)
    pass_on(1)

    def join(cond, name, ref):
        @pl.when(cond)
        def _():
            arrived(name, ref)
            mine[0] += ref[0]
            xout[0] += ref[1]

    join(up(FAR), "g4", g4in)
    join(up(3) & jnp.logical_not(top), "g3", g3in)
    start("gx0", xout.at[0], xin.at[0], across)

    def dq_part(i):
        hi = ds[i, 0]
        return dot(ktcat[i], jnp.concatenate([hi, hi, ds[i, 1]], 0), NN)

    dqt[...] = dq_part(0)
    for i in range(1, STEPS + 1):
        @pl.when(b >= (i if i < STEPS else 1))
        def _():
            dqt[...] += dq_part(i)
    dq_ref[...] = dqt[...].T

    arrived("gx0", xin.at[0])
    dkv_ref[...] = mine[0] + xin[0]


    @pl.when(up(3) & top)
    def _():
        arrived("g3", g3in)
        dkv_ref[...] += g3in[0] + g3in[1]
    for o in ROOT:
        @pl.when(first)
        def _():
            arrived(f"gd{o}", gdin.at[o - 1])
            dkv_ref[...] += gdin[o - 1, 0] + gdin[o - 1, 1]
    for o in (2, 1):
        @pl.when(up(o) & jnp.logical_not(first) if o in ROOT else up(o))
        def _():
            arrived(f"gz{o}", gin.at[o])
            dkv_ref[...] += gin[o]

    @pl.when(first)
    def _():
        arrived("b2", s2in.at[1:ni * no])
        for i in range(ni):
            part = s2in[i * no] if i else s2[...]
            for z in range(1, no):
                part = part + s2in[i * no + z]
            dkv_ref[i * pr:(i + 1) * pr] += part

    one_tile = buf.at[0, 0]
    waits = [
        (None, "all", tally), (up(1), "w1", one_tile), (sends(2), "w2", one_tile),
        (up(3), "w3", buf.at[0]), (up(FAR), "w4", buf.at[0]),
        (down(1), "d1", xout.at[0:3]), (down(2), "d2", xout.at[0:3]),
        (down(3), "g3", g3out), (down(FAR), "g4", g4out),
        (top, "f2", sinkb.at[0:no - 1]), (first, "f1", sin.at[1:2 * ni]),
        (jnp.logical_not(first), "b2", s2),
        (between, "on", one_tile), (bridge, "over", one_tile),
    ]
    assert {w[1] for w in waits} == set(sent_slots), sent_slots
    for cond, name, like in waits:
        when(cond, pltpu.make_async_remote_copy(
            src_ref=like, dst_ref=like, send_sem=send.at[sent_slots[name]], recv_sem=recv.at[0],
            device_id=across, device_id_type=MESH,
        ).wait_send)
    assert len(slots) == recv.shape[0] and len(sent_slots) == send.shape[0]


def store(dq_ref, dkv_ref, dq_hbm, dk_hbm, dv_hbm, sem):
    half = dk_hbm.shape[0]
    moves = [
        (dq_ref, dq_hbm), (dkv_ref.at[0:half], dk_hbm), (dkv_ref.at[half:2 * half], dv_hbm),
    ]
    copies = [pltpu.make_async_copy(x, y, sem.at[i]) for i, (x, y) in enumerate(moves)]
    for c in copies:
        c.start()
    for c in copies:
        c.wait()


def shards(ni, no, queries, key_rows, values, out_grad, sink_len, window_len, block_codes):
    block, heads_dev, dim = queries.shape
    rows = block * heads_dev
    half = key_rows.shape[1]
    codes = block_codes.T
    pr = block // ni
    total = STEPS + 1
    vmem, hbm = pl.BlockSpec(memory_space=pltpu.VMEM), pl.BlockSpec(memory_space=pltpu.HBM)
    tile = (block, dim)
    grad_q, grad_kv = pl.pallas_call(
        functools.partial(kernel, (ni, no, heads_dev)),
        out_shape=(
            pltpu.VMEM((rows, dim), f32),
            pltpu.VMEM((2 * half, block), f32),
        ),
        in_specs=[hbm] * 7,
        out_specs=(vmem,) * 2,
        scratch_shapes=[
            pltpu.SMEM(sink_len.shape, jnp.int32),
            pltpu.SMEM(window_len.shape, jnp.int32),
            pltpu.SMEM(codes.shape, jnp.int32),
            pltpu.VMEM((rows, dim), f32),
            pltpu.VMEM((rows, dim), f32),
            pltpu.SemaphoreType.DMA((7,)),
            pltpu.VMEM((STEPS, 2) + tile, f32),
            pltpu.VMEM((ni, 2, pr, dim), f32),
            pltpu.VMEM((2, pr, dim), f32),
            pltpu.VMEM((rows, 2 * dim), bf16),
            pltpu.VMEM((rows, 2 * dim), bf16),
            pltpu.VMEM((total, block, rows), f32),
            pltpu.VMEM((total, block, rows), f32),
            pltpu.VMEM((8, rows), f32),
            pltpu.VMEM((8, rows), f32),
            pltpu.VMEM((total, 2, block, rows), bf16),
            pltpu.VMEM((total, dim, 3 * block), bf16),
            pltpu.VMEM((DIRECT,) + tile, f32),
            pltpu.VMEM((DIRECT,) + tile, f32),
            pltpu.VMEM((DIRECT,) + tile, f32),
            pltpu.VMEM((DIRECT,) + tile, f32),
            pltpu.VMEM((DIRECT,) + tile, f32),
            pltpu.VMEM((2,) + tile, f32),
            pltpu.VMEM((2,) + tile, f32),
            pltpu.VMEM((2,) + tile, f32),
            pltpu.VMEM((2 * ni, pr, dim), f32),
            pltpu.VMEM((pr, dim), f32),
            pltpu.VMEM((ni * no, pr, dim), f32),
            pltpu.VMEM((dim, rows), f32),
            pltpu.VMEM((2,) + tile, f32),
            pltpu.VMEM((2,) + tile, f32),
            pltpu.VMEM((2, 2) + tile, f32),
            pltpu.VMEM((2 * block + (4 * ni - 3) * pr, dim), f32),
            pltpu.SemaphoreType.DMA((14,)),
            pltpu.SemaphoreType.DMA((21,)),
            pltpu.SemaphoreType.REGULAR((2,)),
        ],
        compiler_params=pltpu.CompilerParams(
            collective_id=0, has_side_effects=True, vmem_limit_bytes=66_000_000
        ),
    )(
        sink_len, window_len, codes,
        queries.reshape(rows, dim), key_rows.T, values.T, out_grad.reshape(rows, dim),
    )
    grad_q, grad_k, grad_v = pl.pallas_call(
        store,
        out_shape=(
            jax.ShapeDtypeStruct((rows, dim), f32),
            jax.ShapeDtypeStruct((half, block), f32),
            jax.ShapeDtypeStruct((half, block), f32),
        ),
        in_specs=[vmem] * 2,
        out_specs=(hbm,) * 3,
        scratch_shapes=[pltpu.SemaphoreType.DMA((3,))],
        compiler_params=pltpu.CompilerParams(vmem_limit_bytes=1 << 20),
    )(grad_q, grad_kv)
    return grad_q.reshape(queries.shape), grad_k.T, grad_v.T


def solution(mesh):
    in_specs = (
        P(("inner", "outer"), "head", None),
        P(("inner", "outer"), "head"),
        P(("inner", "outer"), "head"),
        P(("inner", "outer"), "head", None),
        P(),
        P(),
        P(),
    )
    out_specs = (
        P(("inner", "outer"), "head", None),
        P(("inner", "outer"), "head"),
        P(("inner", "outer"), "head"),
    )
    body = functools.partial(shards, mesh.shape["inner"], mesh.shape["outer"])
    return jax.shard_map(body, mesh=mesh, in_specs=in_specs, out_specs=out_specs, check_vma=False)
```

```python
import functools
import math

import jax
import jax.numpy as jnp
from jax import lax
from jax.experimental import pallas as pl
from jax.experimental.pallas import tpu as pltpu
from jax.sharding import PartitionSpec as P

STEPS = 5
FAR = STEPS - 1
DIRECT = FAR - 1
LATE = (2, 3)
ROOT = (1,)
BIG = 1 << 28
very_low = -1e30
SENT = {
    "x0": "all", "f3": "all", "b1": "all", "gx0": "all", "w3x": "w3", "w4x": "w4",
    "r1": "d1", "gx1": "d1", "gz1": "d1", "gd1": "d1", "r2": "d2", "gx2": "d2", "gz2": "d2",
    "f1_0": "f1", "f1_1": "f1",
}
CAME = {"w3x": "w3", "f1_0": "f1", "f1_1": "f1"}
f32, bf16 = jnp.float32, jnp.bfloat16
MESH = pl.DeviceIdType.MESH
NT = (((1,), (1,)), ((), ()))
NN = (((1,), (0,)), ((), ()))


def dot(a, b, dims):
    return lax.dot_general(a, b, dims, preferred_element_type=f32)


def two(x):
    hi = x.astype(bf16)
    return hi, (x - hi.astype(f32)).astype(bf16)


def when(cond, f):
    if cond is None:
        f()
    else:
        pl.when(cond)(f)


def kernel(
    sizes, sink_hbm, window_hbm, codes_hbm, q_hbm, k_hbm, v_hbm, g_hbm, dq_ref, dkv_ref,
    sink_ref, window_ref, codes_ref, q_ref, g_ref, load, buf, sinkb, piece, qcat, gcat,
    st, dp, peak, run, ds, ktcat, xout, xin, mine, gout, gin, g4out, g4in, sg, sin, s2, s2in,
    dqt, g3out, g3in, gdin, tally, send, recv, late,
):
    ni, no, heads_dev = sizes
    half, block = k_hbm.shape
    rows = q_ref.shape[0]
    temper = 1.0 / math.sqrt(2 * half)
    head, inner, outer = lax.axis_index("head"), lax.axis_index("inner"), lax.axis_index("outer")
    par = lax.rem(head, 2)
    other = 1 - par
    partner = head + 1 - 2 * par
    count = ni * no
    b = inner * no + outer
    pr = block // ni

    def seq(o):
        t = lax.rem(b + o + count, count)
        return (head, t // no, lax.rem(t, no))

    across = (partner, inner, outer)
    columns = [(p, d) for p in range(2) for d in range(ni) if p or d]
    first = (inner == 0) & (outer == 0)
    top = outer == 0

    def column(p, d):
        return (partner if p else head, lax.rem(inner + d, ni), outer)

    def up(o):
        return b + o < count

    def down(o):
        return b >= o

    sent_slots, slots = {}, {}

    def numbered(table, name):
        return table.setdefault(name, len(table))

    def copy(name, src, dst, device, via=None):
        out = numbered(sent_slots, SENT.get(via or name, via or name))
        return pltpu.make_async_remote_copy(
            src_ref=src, dst_ref=dst,
            send_sem=send.at[out], recv_sem=recv.at[numbered(slots, CAME.get(name, name))],
            device_id=device, device_id_type=MESH,
        )

    def start(name, src, dst, device, cond=None, via=None):
        when(cond, copy(name, src, dst, device, via).start)

    def arrived(name, dst):
        pltpu.make_async_remote_copy(
            src_ref=dst, dst_ref=dst, send_sem=send.at[0],
            recv_sem=recv.at[numbered(slots, CAME.get(name, name))],
            device_id=across, device_id_type=MESH,
        ).wait_recv()

    moves = [
        (k_hbm, buf.at[0, par, 0:half]), (v_hbm, buf.at[0, par, half:2 * half]),
        (q_hbm, q_ref), (g_hbm, g_ref),
        (codes_hbm, codes_ref), (sink_hbm, sink_ref), (window_hbm, window_ref),
    ]
    loads = [pltpu.make_async_copy(x, y, load.at[i]) for i, (x, y) in enumerate(moves)]

    barrier = pltpu.get_barrier_semaphore()

    def signal(where, device):
        pl.semaphore_signal(where, inc=1, device_id=device, device_id_type=MESH)

    end = outer == no - 1

    def both(o):
        head_o, inner_o, outer_o = seq(o)
        return [(head, inner_o, outer_o), (partner, inner_o, outer_o)]

    def one(cond, n=1):
        return jnp.where(cond, n, 0)

    far = outer >= 2
    bridged = (lax.rem(inner, 2) == 0) & (inner > 0)
    bridge = far & bridged

    def sends(o):
        if o == 2:
            return up(o) & (top | ((outer + o >= no) & (lax.rem(inner, 2) == 0)))
        return up(o)

    def hears(o):
        if o == 2:
            return down(o) & ((outer == o) | ((outer < o) & (lax.rem(inner, 2) == 1)))
        return down(o)

    signal(barrier, across)
    for d in range(1, ni):
        signal(barrier, column(0, d))
    expect = ni + one(first, ni - 1)
    when(top & (inner != 0), lambda: signal(barrier, (partner, 0, 0)))
    for o in range(1, STEPS):
        asks, tells = sends(o), hears(o)
        if o in LATE:
            asks, tells = asks & (outer != 0), tells & (outer != o)
        when(tells, lambda: signal(barrier, seq(-o)))
        expect = expect + one(asks)
    for o in LATE:
        when(top, lambda: signal(barrier, seq(o)))
    near_bridge = (outer < 2) & bridged
    when(near_bridge, lambda: signal(barrier, seq(2)))
    expect = expect + one(far) + one(bridge)

    for x in loads:
        x.start()
    pl.semaphore_wait(barrier, expect)
    for i, o in enumerate(LATE):
        when(outer == o, lambda: signal(late.at[i], seq(-o)))

    def own_to(name, dst, devices, cond=None):
        for device in devices:
            start(name, k_hbm, dst.at[0:half], device, cond)
            start(name, v_hbm, dst.at[half:2 * half], device, cond)

    def rows_of(i):
        return (k_hbm.at[pl.ds(i * pr, pr)] if i * pr < half
                else v_hbm.at[pl.ds(i * pr - half, pr)])

    for i in range(ni):
        for p in range(2):
            if i or p:
                to = (partner if p else head, i, 0)
                start(f"f1_{p}", rows_of(i), piece.at[par], to, first)

    own_to("x0", buf.at[0, par], [across])
    for o in range(1, STEPS):
        now = sends(o) & (outer != 0) if o in LATE else sends(o)
        own_to(f"w{o}", buf.at[o, par], [seq(o)], now)

    loads[2].wait()
    q0, q1 = two(q_ref[...])
    qcat[...] = jnp.concatenate([q0, q1], 1)
    loads[3].wait()
    g0, g1 = two(g_ref[...])
    gcat[...] = jnp.concatenate([g0, g1], 1)
    for i in (0, 1, 4, 5, 6):
        loads[i].wait()

    @pl.when(first)
    def _():
        piece[par] = buf[0, par, 0:pr, :]

    jk = lax.broadcasted_iota(jnp.int32, (block, rows), 0)
    iq = lax.broadcasted_iota(jnp.int32, (block, rows), 1) // heads_dev
    gap = iq - jk
    sink_end, window = sink_ref[0], window_ref[0]

    def mask_of(o):
        code = codes_ref[o, b]
        limit = jnp.where(code == 2, BIG, jnp.where(code == 1, window, -BIG)) - o * block
        here = jnp.where(b == o, sink_end, 0)
        if o == 0:
            return (gap >= 0) & ((gap < limit) | (jk < here))
        return (gap < limit) & (jk >= here)

    def scores_of(keys, vals, index, allowed):
        k0, k1 = two(keys.T)
        v0, v1 = two(vals.T)
        kk = jnp.concatenate([jnp.concatenate([k0, k0], 1), jnp.concatenate([k1, k1], 1)], 0)
        vv = jnp.concatenate([jnp.concatenate([v0, v0], 1), jnp.concatenate([v1, v1], 1)], 0)
        s = dot(kk, qcat[...], NT)
        s = jnp.where(allowed, temper * (s[0:block] + s[block:]), very_low)
        d = dot(vv, gcat[...], NT)
        d = d[0:block] + d[block:]
        t0, t1 = two(keys * temper)
        ktcat[index] = jnp.concatenate([t0, t1, t0], 1)
        high = jnp.max(s, axis=0, keepdims=True)
        if index:
            before = run[0:1]
            high = jnp.maximum(high, before)
            shrink = jnp.exp(before - high)
        e = jnp.exp(s - high)
        st[index] = e
        dp[index] = d
        norm = jnp.sum(e, axis=0, keepdims=True)
        delta = jnp.sum(e * d, axis=0, keepdims=True)
        if index:
            norm = norm + shrink * run[1:2]
            delta = delta + shrink * run[2:3]
        peak[index:index + 1] = high
        run[0:1] = high
        run[1:2] = norm
        run[2:3] = delta

    def slot(o):
        def _():
            a, c = buf[o, 0], buf[o, 1]
            scores_of(
                jnp.concatenate([a[0:half], c[0:half]], 0),
                jnp.concatenate([a[half:], c[half:]], 0), o, mask_of(o),
            )
        return _

    def relay(o):
        @pl.when(down(o))
        def _():
            arrived(f"w{o}", buf.at[o, par])
            copy(f"r{o}", buf.at[o, par], buf.at[o, par], across).start()

    @pl.when(top)
    def _():
        pl.semaphore_wait(late.at[0], 1)
        own_to("w2", buf.at[2, par], [seq(2)])

        @pl.when(jnp.logical_not(first))
        def _():
            arrived("f1", piece)

        @pl.when(first)
        def _():
            arrived("f1", piece.at[other])
        start("f2", piece, piece, (head, inner, 1))
        pl.semaphore_wait(late.at[1], 1)
        for z in range(no - 1, 1, -1):
            start("f2", piece, piece, (head, inner, z))
        own_to("w3", buf.at[3, par], [seq(3)])

    @pl.when(outer != 0)
    def _():
        relay(1)

    between = outer == no - 2
    start("w2", buf.at[1, par], buf.at[2, par], seq(1), between, "on")

    @pl.when(bridge)
    def _():
        arrived(f"w{FAR}", buf.at[FAR, par])
    start("w2", buf.at[FAR, par], buf.at[2, par], seq(-2), bridge, "over")

    arrived("x0", buf.at[0, other])
    start("w3x", buf.at[0, other], buf.at[3, other], seq(3), up(3))
    start("w4x", buf.at[0, other], buf.at[FAR, other], seq(FAR), up(FAR))

    def spread():
        for d in range(1, ni):
            start("f3", piece, sinkb.at[inner], column(0, d))
        sinkb[inner] = piece[...]

    def sink():
        arrived("f2", piece)
        spread()

    slot(0)()

    @pl.when(top)
    def _():
        spread()

        @pl.when(bridged)
        def _():
            relay(1)
            relay(2)

        @pl.when(jnp.logical_not(bridged))
        def _():
            relay(2)
            relay(1)

    @pl.when(outer == 1)
    def _():
        sink()
        relay(2)

    @pl.when(outer > 1)
    def _():
        relay(2)
        sink()

    @pl.when(down(FAR))
    def _():
        @pl.when(jnp.logical_not(bridge))
        def _():
            arrived(f"w{FAR}", buf.at[FAR, par])
        arrived("w4x", buf.at[FAR, other])
        slot(FAR)()

    def last(o):
        @pl.when(down(o))
        def _():
            arrived(f"r{o}", buf.at[o, other])
            slot(o)()

    def sinks():
        arrived("f3", sinkb.at[0:ni - 1])

        @pl.when(b >= 1)
        def _():
            a = [sinkb[i, p] for p in range(2) for i in range(ni)]
            cut = ni // 2
            keys = jnp.concatenate(a[0:cut] + a[ni:ni + cut], 0)
            vals = jnp.concatenate(a[cut:ni] + a[ni + cut:], 0)
            scores_of(keys, vals, STEPS, jk < sink_end)

    def third():
        @pl.when(down(3))
        def _():
            arrived("w3", buf.at[3])
            slot(3)()

    @pl.when(top)
    def _():
        third()
        sinks()

        @pl.when(bridged)
        def _():
            last(1)
            last(2)

        @pl.when(jnp.logical_not(bridged))
        def _():
            last(2)
            last(1)

    @pl.when((outer != 0) & jnp.logical_not(end))
    def _():
        third()
        last(1)
        last(2)
        sinks()

    @pl.when(end)
    def _():
        last(1)
        last(2)
        sinks()
        third()

    high = run[0:1]
    scale = 1.0 / run[1:2]
    delta = run[2:3] * scale

    def grads(i):
        probs = st[i] * (jnp.exp(peak[i:i + 1] - high) * scale)
        score = probs * (dp[i] - delta)
        p_hi, p_lo = two(probs)
        d_hi, d_lo = two(score)
        ds[i, 0] = d_hi
        ds[i, 1] = d_lo
        w = 2 * half
        pv = dot(jnp.concatenate([p_hi, p_lo], 0), gcat[...], NN)
        dv = pv[0:block, 0:w] + pv[0:block, w:] + pv[block:, 0:w]
        kq = dot(jnp.concatenate([d_hi, d_lo], 0), qcat[...], NN)
        dk = temper * (kq[0:block, 0:w] + kq[0:block, w:] + kq[block:, 0:w])
        dk, dv = dk.T, dv.T
        even = jnp.concatenate([dk[0:half], dv[0:half]], 0)
        odd = jnp.concatenate([dk[half:], dv[half:]], 0)
        keep = jnp.where(par == 0, even, odd)
        give = jnp.where(par == 0, odd, even)
        return keep, give

    def at_root(o):
        return b == (o if o in ROOT else -1)

    def give_near(o):
        @pl.when(down(o))
        def _():
            keep, give = grads(o)
            mine[o] = keep
            xout[o] = give
        c = copy(f"gx{o}", xout.at[o], xin.at[o], across)
        when(down(o) & (~at_root(o)), c.start)
        if o not in ROOT:
            return
        start(f"gd{o}", mine.at[o], gdin.at[o - 1, 0], (head, 0, 0), at_root(o))
        start(f"gd{o}", xout.at[o], gdin.at[o - 1, 1], (partner, 0, 0), at_root(o))

    def pass_on(o):
        @pl.when(down(o) & (~at_root(o)))
        def _():
            arrived(f"gx{o}", xin.at[o])
            gout[o] = mine[o] + xin[o]
        c = copy(f"gz{o}", gout.at[o], gin.at[o], seq(-o))
        when(down(o) & (~at_root(o)), c.start)

    @pl.when(((outer == 2) & (2 * inner < ni)))
    def _():
        give_near(2)

    @pl.when(b >= 1)
    def _():
        keep, give = grads(STEPS)
        sg[0] = keep
        sg[1] = give

    @pl.when(b == 0)
    def _():
        sg[...] = jnp.zeros_like(sg)

    for p, d in columns[::-1]:
        target = lax.rem(inner + d, ni)
        rng = pl.ds(pl.multiple_of(target * pr, pr), pr)
        start("b1", sg.at[p, rng], sin.at[p * ni + d], column(p, d))

    @pl.when(down(3))
    def _():
        keep, give = grads(3)
        g3out[0] = keep
        g3out[1] = give
    for p, device in enumerate(both(-3)):
        start("g3", g3out.at[p], g3in.at[p], device, down(3) & end if p else down(3))
    start("g3", g3out.at[1], g3in.at[1], seq(-3), down(3) & jnp.logical_not(end))

    @pl.when(jnp.logical_not(((outer == 2) & (2 * inner < ni))))
    def _():
        give_near(2)
    give_near(1)

    @pl.when(down(FAR))
    def _():
        keep, give = grads(FAR)
        g4out[0] = keep
        g4out[1] = give
    start("g4", g4out, g4in, seq(-FAR), down(FAR))

    keep, give = grads(0)
    mine[0] = keep
    xout[0] = give

    where = pl.ds(pl.multiple_of(inner * pr, pr), pr)
    @pl.when(((outer == 2) & (2 * inner < ni)))
    def _():
        pass_on(2)
    arrived("b1", sin.at[1:2 * ni])
    acc = sg[0, where]
    for p, d in columns:
        acc = acc + sin[p * ni + d]
    s2[...] = acc
    for i in range(ni):
        for z in range(no):
            if i or z:
                mine_here = (inner == i) & (outer == z)
                start("b2", s2, s2in.at[i * no + z], (head, 0, 0), mine_here)

    @pl.when(jnp.logical_not(((outer == 2) & (2 * inner < ni))))
    def _():
        pass_on(2)
    pass_on(1)

    def join(cond, name, ref):
        @pl.when(cond)
        def _():
            arrived(name, ref)
            mine[0] += ref[0]
            xout[0] += ref[1]

    join(up(FAR), "g4", g4in)
    join(up(3) & jnp.logical_not(top), "g3", g3in)
    start("gx0", xout.at[0], xin.at[0], across)

    def dq_part(i):
        hi = ds[i, 0]
        return dot(ktcat[i], jnp.concatenate([hi, hi, ds[i, 1]], 0), NN)

    dqt[...] = dq_part(0)
    for i in range(1, STEPS + 1):
        @pl.when(b >= (i if i < STEPS else 1))
        def _():
            dqt[...] += dq_part(i)
    dq_ref[...] = dqt[...].T

    arrived("gx0", xin.at[0])
    dkv_ref[...] = mine[0] + xin[0]


    @pl.when(up(3) & top)
    def _():
        arrived("g3", g3in)
        dkv_ref[...] += g3in[0] + g3in[1]
    for o in ROOT:
        @pl.when(first)
        def _():
            arrived(f"gd{o}", gdin.at[o - 1])
            dkv_ref[...] += gdin[o - 1, 0] + gdin[o - 1, 1]
    for o in (2, 1):
        @pl.when(up(o) & jnp.logical_not(first) if o in ROOT else up(o))
        def _():
            arrived(f"gz{o}", gin.at[o])
            dkv_ref[...] += gin[o]

    @pl.when(first)
    def _():
        arrived("b2", s2in.at[1:ni * no])
        for i in range(ni):
            part = s2in[i * no] if i else s2[...]
            for z in range(1, no):
                part = part + s2in[i * no + z]
            dkv_ref[i * pr:(i + 1) * pr] += part

    one_tile = buf.at[0, 0]
    waits = [
        (None, "all", tally), (up(1), "w1", one_tile), (sends(2), "w2", one_tile),
        (up(3), "w3", buf.at[0]), (up(FAR), "w4", buf.at[0]),
        (down(1), "d1", xout.at[0:3]), (down(2), "d2", xout.at[0:3]),
        (down(3), "g3", g3out), (down(FAR), "g4", g4out),
        (top, "f2", sinkb.at[0:no - 1]), (first, "f1", sin.at[1:2 * ni]),
        (jnp.logical_not(first), "b2", s2),
        (between, "on", one_tile), (bridge, "over", one_tile),
    ]
    assert {w[1] for w in waits} == set(sent_slots), sent_slots
    for cond, name, like in waits:
        when(cond, pltpu.make_async_remote_copy(
            src_ref=like, dst_ref=like, send_sem=send.at[sent_slots[name]], recv_sem=recv.at[0],
            device_id=across, device_id_type=MESH,
        ).wait_send)
    assert len(slots) == recv.shape[0] and len(sent_slots) == send.shape[0]


def store(dq_ref, dkv_ref, dq_hbm, dk_hbm, dv_hbm, sem):
    half = dk_hbm.shape[0]
    moves = [
        (dq_ref, dq_hbm), (dkv_ref.at[0:half], dk_hbm), (dkv_ref.at[half:2 * half], dv_hbm),
    ]
    copies = [pltpu.make_async_copy(x, y, sem.at[i]) for i, (x, y) in enumerate(moves)]
    for c in copies:
        c.start()
    for c in copies:
        c.wait()


def shards(ni, no, queries, key_rows, values, out_grad, sink_len, window_len, block_codes):
    block, heads_dev, dim = queries.shape
    rows = block * heads_dev
    half = key_rows.shape[1]
    codes = block_codes.T
    pr = block // ni
    total = STEPS + 1
    vmem, hbm = pl.BlockSpec(memory_space=pltpu.VMEM), pl.BlockSpec(memory_space=pltpu.HBM)
    tile = (block, dim)
    grad_q, grad_kv = pl.pallas_call(
        functools.partial(kernel, (ni, no, heads_dev)),
        out_shape=(
            pltpu.VMEM((rows, dim), f32),
            pltpu.VMEM((2 * half, block), f32),
        ),
        in_specs=[hbm] * 7,
        out_specs=(vmem,) * 2,
        scratch_shapes=[
            pltpu.SMEM(sink_len.shape, jnp.int32),
            pltpu.SMEM(window_len.shape, jnp.int32),
            pltpu.SMEM(codes.shape, jnp.int32),
            pltpu.VMEM((rows, dim), f32),
            pltpu.VMEM((rows, dim), f32),
            pltpu.SemaphoreType.DMA((7,)),
            pltpu.VMEM((STEPS, 2) + tile, f32),
            pltpu.VMEM((ni, 2, pr, dim), f32),
            pltpu.VMEM((2, pr, dim), f32),
            pltpu.VMEM((rows, 2 * dim), bf16),
            pltpu.VMEM((rows, 2 * dim), bf16),
            pltpu.VMEM((total, block, rows), f32),
            pltpu.VMEM((total, block, rows), f32),
            pltpu.VMEM((8, rows), f32),
            pltpu.VMEM((8, rows), f32),
            pltpu.VMEM((total, 2, block, rows), bf16),
            pltpu.VMEM((total, dim, 3 * block), bf16),
            pltpu.VMEM((DIRECT,) + tile, f32),
            pltpu.VMEM((DIRECT,) + tile, f32),
            pltpu.VMEM((DIRECT,) + tile, f32),
            pltpu.VMEM((DIRECT,) + tile, f32),
            pltpu.VMEM((DIRECT,) + tile, f32),
            pltpu.VMEM((2,) + tile, f32),
            pltpu.VMEM((2,) + tile, f32),
            pltpu.VMEM((2,) + tile, f32),
            pltpu.VMEM((2 * ni, pr, dim), f32),
            pltpu.VMEM((pr, dim), f32),
            pltpu.VMEM((ni * no, pr, dim), f32),
            pltpu.VMEM((dim, rows), f32),
            pltpu.VMEM((2,) + tile, f32),
            pltpu.VMEM((2,) + tile, f32),
            pltpu.VMEM((2, 2) + tile, f32),
            pltpu.VMEM((2 * block + (4 * ni - 3) * pr, dim), f32),
            pltpu.SemaphoreType.DMA((14,)),
            pltpu.SemaphoreType.DMA((21,)),
            pltpu.SemaphoreType.REGULAR((2,)),
        ],
        compiler_params=pltpu.CompilerParams(
            collective_id=0, has_side_effects=True, vmem_limit_bytes=66_000_000
        ),
    )(
        sink_len, window_len, codes,
        queries.reshape(rows, dim), key_rows.T, values.T, out_grad.reshape(rows, dim),
    )
    grad_q, grad_k, grad_v = pl.pallas_call(
        store,
        out_shape=(
            jax.ShapeDtypeStruct((rows, dim), f32),
            jax.ShapeDtypeStruct((half, block), f32),
            jax.ShapeDtypeStruct((half, block), f32),
        ),
        in_specs=[vmem] * 2,
        out_specs=(hbm,) * 3,
        scratch_shapes=[pltpu.SemaphoreType.DMA((3,))],
        compiler_params=pltpu.CompilerParams(vmem_limit_bytes=1 << 20),
    )(grad_q, grad_kv)
    return grad_q.reshape(queries.shape), grad_k.T, grad_v.T


def solution(mesh):
    in_specs = (
        P(("inner", "outer"), "head", None),
        P(("inner", "outer"), "head"),
        P(("inner", "outer"), "head"),
        P(("inner", "outer"), "head", None),
        P(),
        P(),
        P(),
    )
    out_specs = (
        P(("inner", "outer"), "head", None),
        P(("inner", "outer"), "head"),
        P(("inner", "outer"), "head"),
    )
    body = functools.partial(shards, mesh.shape["inner"], mesh.shape["outer"])
    return jax.shard_map(body, mesh=mesh, in_specs=in_specs, out_specs=out_specs, check_vma=False)
```

```python
import functools
import math

import jax
import jax.numpy as jnp
from jax import lax
from jax.experimental import pallas as pl
from jax.experimental.pallas import tpu as pltpu
from jax.sharding import PartitionSpec as P

STEPS = 5
FAR = STEPS - 1
DIRECT = FAR - 1
LATE = (2, 3)
ROOT = (1,)
BIG = 1 << 28
very_low = -1e30
SENT = {
    "x0": "all", "f3": "all", "b1": "all", "gx0": "all", "w3x": "w3", "w4x": "w4",
    "r1": "d1", "gx1": "d1", "gz1": "d1", "gd1": "d1", "r2": "d2", "gx2": "d2", "gz2": "d2",
    "f1_0": "f1", "f1_1": "f1",
}
CAME = {"w3x": "w3", "f1_0": "f1", "f1_1": "f1"}
f32, bf16 = jnp.float32, jnp.bfloat16
MESH = pl.DeviceIdType.MESH
NT = (((1,), (1,)), ((), ()))
NN = (((1,), (0,)), ((), ()))


def dot(a, b, dims):
    return lax.dot_general(a, b, dims, preferred_element_type=f32)


def two(x):
    hi = x.astype(bf16)
    return hi, (x - hi.astype(f32)).astype(bf16)


def when(cond, f):
    if cond is None:
        f()
    else:
        pl.when(cond)(f)


def kernel(
    sizes, sink_hbm, window_hbm, codes_hbm, q_hbm, k_hbm, v_hbm, g_hbm, dq_ref, dkv_ref,
    sink_ref, window_ref, codes_ref, q_ref, g_ref, load, buf, sinkb, piece, qcat, gcat,
    st, dp, peak, run, ds, ktcat, xout, xin, mine, gout, gin, g4out, g4in, sg, sin, s2, s2in,
    dqt, g3out, g3in, gdin, tally, send, recv, late,
):
    ni, no, heads_dev = sizes
    half, block = k_hbm.shape
    rows = q_ref.shape[0]
    temper = 1.0 / math.sqrt(2 * half)
    head, inner, outer = lax.axis_index("head"), lax.axis_index("inner"), lax.axis_index("outer")
    par = lax.rem(head, 2)
    other = 1 - par
    partner = head + 1 - 2 * par
    count = ni * no
    b = inner * no + outer
    pr = block // ni

    def seq(o):
        t = lax.rem(b + o + count, count)
        return (head, t // no, lax.rem(t, no))

    across = (partner, inner, outer)
    columns = [(p, d) for p in range(2) for d in range(ni) if p or d]
    first = (inner == 0) & (outer == 0)
    top = outer == 0

    def column(p, d):
        return (partner if p else head, lax.rem(inner + d, ni), outer)

    def up(o):
        return b + o < count

    def down(o):
        return b >= o

    sent_slots, slots = {}, {}

    def numbered(table, name):
        return table.setdefault(name, len(table))

    def copy(name, src, dst, device, via=None):
        out = numbered(sent_slots, SENT.get(via or name, via or name))
        return pltpu.make_async_remote_copy(
            src_ref=src, dst_ref=dst,
            send_sem=send.at[out], recv_sem=recv.at[numbered(slots, CAME.get(name, name))],
            device_id=device, device_id_type=MESH,
        )

    def start(name, src, dst, device, cond=None, via=None):
        when(cond, copy(name, src, dst, device, via).start)

    def arrived(name, dst):
        pltpu.make_async_remote_copy(
            src_ref=dst, dst_ref=dst, send_sem=send.at[0],
            recv_sem=recv.at[numbered(slots, CAME.get(name, name))],
            device_id=across, device_id_type=MESH,
        ).wait_recv()

    moves = [
        (k_hbm, buf.at[0, par, 0:half]), (v_hbm, buf.at[0, par, half:2 * half]),
        (q_hbm, q_ref), (g_hbm, g_ref),
        (codes_hbm, codes_ref), (sink_hbm, sink_ref), (window_hbm, window_ref),
    ]
    loads = [pltpu.make_async_copy(x, y, load.at[i]) for i, (x, y) in enumerate(moves)]

    barrier = pltpu.get_barrier_semaphore()

    def signal(where, device):
        pl.semaphore_signal(where, inc=1, device_id=device, device_id_type=MESH)

    end = outer == no - 1

    def both(o):
        head_o, inner_o, outer_o = seq(o)
        return [(head, inner_o, outer_o), (partner, inner_o, outer_o)]

    def one(cond, n=1):
        return jnp.where(cond, n, 0)

    far = outer >= 2
    bridged = (lax.rem(inner, 2) == 0) & (inner > 0)
    bridge = far & bridged

    def sends(o):
        if o == 2:
            return up(o) & (top | ((outer + o >= no) & (lax.rem(inner, 2) == 0)))
        return up(o)

    def hears(o):
        if o == 2:
            return down(o) & ((outer == o) | ((outer < o) & (lax.rem(inner, 2) == 1)))
        return down(o)

    signal(barrier, across)
    for d in range(1, ni):
        signal(barrier, column(0, d))
    expect = ni + one(first, ni - 1)
    when(top & (inner != 0), lambda: signal(barrier, (partner, 0, 0)))
    for o in range(1, STEPS):
        asks, tells = sends(o), hears(o)
        if o in LATE:
            asks, tells = asks & (outer != 0), tells & (outer != o)
        when(tells, lambda: signal(barrier, seq(-o)))
        expect = expect + one(asks)
    for o in LATE:
        when(top, lambda: signal(barrier, seq(o)))
    near_bridge = (outer < 2) & bridged
    when(near_bridge, lambda: signal(barrier, seq(2)))
    expect = expect + one(far) + one(bridge)

    for x in loads:
        x.start()
    pl.semaphore_wait(barrier, expect)
    for i, o in enumerate(LATE):
        when(outer == o, lambda: signal(late.at[i], seq(-o)))

    def own_to(name, dst, devices, cond=None):
        for device in devices:
            start(name, k_hbm, dst.at[0:half], device, cond)
            start(name, v_hbm, dst.at[half:2 * half], device, cond)

    def rows_of(i):
        return (k_hbm.at[pl.ds(i * pr, pr)] if i * pr < half
                else v_hbm.at[pl.ds(i * pr - half, pr)])

    for i in range(ni):
        for p in range(2):
            if i or p:
                to = (partner if p else head, i, 0)
                start(f"f1_{p}", rows_of(i), piece.at[par], to, first)

    own_to("x0", buf.at[0, par], [across])
    for o in range(1, STEPS):
        now = sends(o) & (outer != 0) if o in LATE else sends(o)
        own_to(f"w{o}", buf.at[o, par], [seq(o)], now)

    loads[2].wait()
    q0, q1 = two(q_ref[...])
    qcat[...] = jnp.concatenate([q0, q1], 1)
    loads[3].wait()
    g0, g1 = two(g_ref[...])
    gcat[...] = jnp.concatenate([g0, g1], 1)
    for i in (0, 1, 4, 5, 6):
        loads[i].wait()

    @pl.when(first)
    def _():
        piece[par] = buf[0, par, 0:pr, :]

    jk = lax.broadcasted_iota(jnp.int32, (block, rows), 0)
    iq = lax.broadcasted_iota(jnp.int32, (block, rows), 1) // heads_dev
    gap = iq - jk
    sink_end, window = sink_ref[0], window_ref[0]

    def mask_of(o):
        code = codes_ref[o, b]
        limit = jnp.where(code == 2, BIG, jnp.where(code == 1, window, -BIG)) - o * block
        here = jnp.where(b == o, sink_end, 0)
        if o == 0:
            return (gap >= 0) & ((gap < limit) | (jk < here))
        return (gap < limit) & (jk >= here)

    def scores_of(keys, vals, index, allowed):
        k0, k1 = two(keys.T)
        v0, v1 = two(vals.T)
        kk = jnp.concatenate([jnp.concatenate([k0, k0], 1), jnp.concatenate([k1, k1], 1)], 0)
        vv = jnp.concatenate([jnp.concatenate([v0, v0], 1), jnp.concatenate([v1, v1], 1)], 0)
        s = dot(kk, qcat[...], NT)
        s = jnp.where(allowed, temper * (s[0:block] + s[block:]), very_low)
        d = dot(vv, gcat[...], NT)
        d = d[0:block] + d[block:]
        t0, t1 = two(keys * temper)
        ktcat[index] = jnp.concatenate([t0, t1, t0], 1)
        high = jnp.max(s, axis=0, keepdims=True)
        if index:
            before = run[0:1]
            high = jnp.maximum(high, before)
            shrink = jnp.exp(before - high)
        e = jnp.exp(s - high)
        st[index] = e
        dp[index] = d
        norm = jnp.sum(e, axis=0, keepdims=True)
        delta = jnp.sum(e * d, axis=0, keepdims=True)
        if index:
            norm = norm + shrink * run[1:2]
            delta = delta + shrink * run[2:3]
        peak[index:index + 1] = high
        run[0:1] = high
        run[1:2] = norm
        run[2:3] = delta

    def slot(o):
        def _():
            a, c = buf[o, 0], buf[o, 1]
            scores_of(
                jnp.concatenate([a[0:half], c[0:half]], 0),
                jnp.concatenate([a[half:], c[half:]], 0), o, mask_of(o),
            )
        return _

    def relay(o):
        @pl.when(down(o))
        def _():
            arrived(f"w{o}", buf.at[o, par])
            copy(f"r{o}", buf.at[o, par], buf.at[o, par], across).start()

    @pl.when(top)
    def _():
        pl.semaphore_wait(late.at[0], 1)
        own_to("w2", buf.at[2, par], [seq(2)])

        @pl.when(jnp.logical_not(first))
        def _():
            arrived("f1", piece)

        @pl.when(first)
        def _():
            arrived("f1", piece.at[other])
        start("f2", piece, piece, (head, inner, 1))
        pl.semaphore_wait(late.at[1], 1)
        for z in range(no - 1, 1, -1):
            start("f2", piece, piece, (head, inner, z))
        own_to("w3", buf.at[3, par], [seq(3)])

    @pl.when(outer != 0)
    def _():
        relay(1)

    between = outer == no - 2
    start("w2", buf.at[1, par], buf.at[2, par], seq(1), between, "on")

    @pl.when(bridge)
    def _():
        arrived(f"w{FAR}", buf.at[FAR, par])
    start("w2", buf.at[FAR, par], buf.at[2, par], seq(-2), bridge, "over")

    arrived("x0", buf.at[0, other])
    start("w3x", buf.at[0, other], buf.at[3, other], seq(3), up(3))
    start("w4x", buf.at[0, other], buf.at[FAR, other], seq(FAR), up(FAR))

    def spread():
        for d in range(1, ni):
            start("f3", piece, sinkb.at[inner], column(0, d))
        sinkb[inner] = piece[...]

    def sink():
        arrived("f2", piece)
        spread()

    slot(0)()

    @pl.when(top)
    def _():
        spread()

        @pl.when(bridged)
        def _():
            relay(1)
            relay(2)

        @pl.when(jnp.logical_not(bridged))
        def _():
            relay(2)
            relay(1)

    @pl.when(outer == 1)
    def _():
        sink()
        relay(2)

    @pl.when(outer > 1)
    def _():
        relay(2)
        sink()

    @pl.when(down(FAR))
    def _():
        @pl.when(jnp.logical_not(bridge))
        def _():
            arrived(f"w{FAR}", buf.at[FAR, par])
        arrived("w4x", buf.at[FAR, other])
        slot(FAR)()

    def last(o):
        @pl.when(down(o))
        def _():
            arrived(f"r{o}", buf.at[o, other])
            slot(o)()

    def sinks():
        arrived("f3", sinkb.at[0:ni - 1])

        @pl.when(b >= 1)
        def _():
            a = [sinkb[i, p] for p in range(2) for i in range(ni)]
            cut = ni // 2
            keys = jnp.concatenate(a[0:cut] + a[ni:ni + cut], 0)
            vals = jnp.concatenate(a[cut:ni] + a[ni + cut:], 0)
            scores_of(keys, vals, STEPS, jk < sink_end)

    def third():
        @pl.when(down(3))
        def _():
            arrived("w3", buf.at[3])
            slot(3)()

    @pl.when(top)
    def _():
        third()
        sinks()

        @pl.when(bridged)
        def _():
            last(1)
            last(2)

        @pl.when(jnp.logical_not(bridged))
        def _():
            last(2)
            last(1)

    @pl.when((outer != 0) & jnp.logical_not(end))
    def _():
        third()
        last(1)

        @pl.when(bridged & (outer == 1))
        def _():
            sinks()
            last(2)

        @pl.when(jnp.logical_not(bridged & (outer == 1)))
        def _():
            last(2)
            sinks()

    @pl.when(end)
    def _():
        last(1)
        last(2)
        sinks()
        third()

    high = run[0:1]
    scale = 1.0 / run[1:2]
    delta = run[2:3] * scale

    def grads(i):
        probs = st[i] * (jnp.exp(peak[i:i + 1] - high) * scale)
        score = probs * (dp[i] - delta)
        p_hi, p_lo = two(probs)
        d_hi, d_lo = two(score)
        ds[i, 0] = d_hi
        ds[i, 1] = d_lo
        w = 2 * half
        pv = dot(jnp.concatenate([p_hi, p_lo], 0), gcat[...], NN)
        dv = pv[0:block, 0:w] + pv[0:block, w:] + pv[block:, 0:w]
        kq = dot(jnp.concatenate([d_hi, d_lo], 0), qcat[...], NN)
        dk = temper * (kq[0:block, 0:w] + kq[0:block, w:] + kq[block:, 0:w])
        dk, dv = dk.T, dv.T
        even = jnp.concatenate([dk[0:half], dv[0:half]], 0)
        odd = jnp.concatenate([dk[half:], dv[half:]], 0)
        keep = jnp.where(par == 0, even, odd)
        give = jnp.where(par == 0, odd, even)
        return keep, give

    def at_root(o):
        return b == (o if o in ROOT else -1)

    def give_near(o):
        @pl.when(down(o))
        def _():
            keep, give = grads(o)
            mine[o] = keep
            xout[o] = give
        c = copy(f"gx{o}", xout.at[o], xin.at[o], across)
        when(down(o) & (~at_root(o)), c.start)
        if o not in ROOT:
            return
        start(f"gd{o}", mine.at[o], gdin.at[o - 1, 0], (head, 0, 0), at_root(o))
        start(f"gd{o}", xout.at[o], gdin.at[o - 1, 1], (partner, 0, 0), at_root(o))

    def pass_on(o):
        @pl.when(down(o) & (~at_root(o)))
        def _():
            arrived(f"gx{o}", xin.at[o])
            gout[o] = mine[o] + xin[o]
        c = copy(f"gz{o}", gout.at[o], gin.at[o], seq(-o))
        when(down(o) & (~at_root(o)), c.start)

    @pl.when(((outer == 2) & (2 * inner < ni)))
    def _():
        give_near(2)

    @pl.when(b >= 1)
    def _():
        keep, give = grads(STEPS)
        sg[0] = keep
        sg[1] = give

    @pl.when(b == 0)
    def _():
        sg[...] = jnp.zeros_like(sg)

    for p, d in columns[::-1]:
        target = lax.rem(inner + d, ni)
        rng = pl.ds(pl.multiple_of(target * pr, pr), pr)
        start("b1", sg.at[p, rng], sin.at[p * ni + d], column(p, d))

    @pl.when(down(3))
    def _():
        keep, give = grads(3)
        g3out[0] = keep
        g3out[1] = give
    for p, device in enumerate(both(-3)):
        start("g3", g3out.at[p], g3in.at[p], device, down(3) & end if p else down(3))
    start("g3", g3out.at[1], g3in.at[1], seq(-3), down(3) & jnp.logical_not(end))

    @pl.when(jnp.logical_not(((outer == 2) & (2 * inner < ni))))
    def _():
        give_near(2)
    give_near(1)

    @pl.when(down(FAR))
    def _():
        keep, give = grads(FAR)
        g4out[0] = keep
        g4out[1] = give
    start("g4", g4out, g4in, seq(-FAR), down(FAR))

    keep, give = grads(0)
    mine[0] = keep
    xout[0] = give

    where = pl.ds(pl.multiple_of(inner * pr, pr), pr)
    @pl.when(((outer == 2) & (2 * inner < ni)))
    def _():
        pass_on(2)
    arrived("b1", sin.at[1:2 * ni])
    acc = sg[0, where]
    for p, d in columns:
        acc = acc + sin[p * ni + d]
    s2[...] = acc
    for i in range(ni):
        for z in range(no):
            if i or z:
                mine_here = (inner == i) & (outer == z)
                start("b2", s2, s2in.at[i * no + z], (head, 0, 0), mine_here)

    @pl.when(jnp.logical_not(((outer == 2) & (2 * inner < ni))))
    def _():
        pass_on(2)
    pass_on(1)

    def join(cond, name, ref):
        @pl.when(cond)
        def _():
            arrived(name, ref)
            mine[0] += ref[0]
            xout[0] += ref[1]

    join(up(FAR), "g4", g4in)
    join(up(3) & jnp.logical_not(top), "g3", g3in)
    start("gx0", xout.at[0], xin.at[0], across)

    def dq_part(i):
        hi = ds[i, 0]
        return dot(ktcat[i], jnp.concatenate([hi, hi, ds[i, 1]], 0), NN)

    dqt[...] = dq_part(0)
    for i in range(1, STEPS + 1):
        @pl.when(b >= (i if i < STEPS else 1))
        def _():
            dqt[...] += dq_part(i)
    dq_ref[...] = dqt[...].T

    arrived("gx0", xin.at[0])
    dkv_ref[...] = mine[0] + xin[0]


    @pl.when(up(3) & top)
    def _():
        arrived("g3", g3in)
        dkv_ref[...] += g3in[0] + g3in[1]
    for o in ROOT:
        @pl.when(first)
        def _():
            arrived(f"gd{o}", gdin.at[o - 1])
            dkv_ref[...] += gdin[o - 1, 0] + gdin[o - 1, 1]
    for o in (2, 1):
        @pl.when(up(o) & jnp.logical_not(first) if o in ROOT else up(o))
        def _():
            arrived(f"gz{o}", gin.at[o])
            dkv_ref[...] += gin[o]

    @pl.when(first)
    def _():
        arrived("b2", s2in.at[1:ni * no])
        for i in range(ni):
            part = s2in[i * no] if i else s2[...]
            for z in range(1, no):
                part = part + s2in[i * no + z]
            dkv_ref[i * pr:(i + 1) * pr] += part

    one_tile = buf.at[0, 0]
    waits = [
        (None, "all", tally), (up(1), "w1", one_tile), (sends(2), "w2", one_tile),
        (up(3), "w3", buf.at[0]), (up(FAR), "w4", buf.at[0]),
        (down(1), "d1", xout.at[0:3]), (down(2), "d2", xout.at[0:3]),
        (down(3), "g3", g3out), (down(FAR), "g4", g4out),
        (top, "f2", sinkb.at[0:no - 1]), (first, "f1", sin.at[1:2 * ni]),
        (jnp.logical_not(first), "b2", s2),
        (between, "on", one_tile), (bridge, "over", one_tile),
    ]
    assert {w[1] for w in waits} == set(sent_slots), sent_slots
    for cond, name, like in waits:
        when(cond, pltpu.make_async_remote_copy(
            src_ref=like, dst_ref=like, send_sem=send.at[sent_slots[name]], recv_sem=recv.at[0],
            device_id=across, device_id_type=MESH,
        ).wait_send)
    assert len(slots) == recv.shape[0] and len(sent_slots) == send.shape[0]


def store(dq_ref, dkv_ref, dq_hbm, dk_hbm, dv_hbm, sem):
    half = dk_hbm.shape[0]
    moves = [
        (dq_ref, dq_hbm), (dkv_ref.at[0:half], dk_hbm), (dkv_ref.at[half:2 * half], dv_hbm),
    ]
    copies = [pltpu.make_async_copy(x, y, sem.at[i]) for i, (x, y) in enumerate(moves)]
    for c in copies:
        c.start()
    for c in copies:
        c.wait()


def shards(ni, no, queries, key_rows, values, out_grad, sink_len, window_len, block_codes):
    block, heads_dev, dim = queries.shape
    rows = block * heads_dev
    half = key_rows.shape[1]
    codes = block_codes.T
    pr = block // ni
    total = STEPS + 1
    vmem, hbm = pl.BlockSpec(memory_space=pltpu.VMEM), pl.BlockSpec(memory_space=pltpu.HBM)
    tile = (block, dim)
    grad_q, grad_kv = pl.pallas_call(
        functools.partial(kernel, (ni, no, heads_dev)),
        out_shape=(
            pltpu.VMEM((rows, dim), f32),
            pltpu.VMEM((2 * half, block), f32),
        ),
        in_specs=[hbm] * 7,
        out_specs=(vmem,) * 2,
        scratch_shapes=[
            pltpu.SMEM(sink_len.shape, jnp.int32),
            pltpu.SMEM(window_len.shape, jnp.int32),
            pltpu.SMEM(codes.shape, jnp.int32),
            pltpu.VMEM((rows, dim), f32),
            pltpu.VMEM((rows, dim), f32),
            pltpu.SemaphoreType.DMA((7,)),
            pltpu.VMEM((STEPS, 2) + tile, f32),
            pltpu.VMEM((ni, 2, pr, dim), f32),
            pltpu.VMEM((2, pr, dim), f32),
            pltpu.VMEM((rows, 2 * dim), bf16),
            pltpu.VMEM((rows, 2 * dim), bf16),
            pltpu.VMEM((total, block, rows), f32),
            pltpu.VMEM((total, block, rows), f32),
            pltpu.VMEM((8, rows), f32),
            pltpu.VMEM((8, rows), f32),
            pltpu.VMEM((total, 2, block, rows), bf16),
            pltpu.VMEM((total, dim, 3 * block), bf16),
            pltpu.VMEM((DIRECT,) + tile, f32),
            pltpu.VMEM((DIRECT,) + tile, f32),
            pltpu.VMEM((DIRECT,) + tile, f32),
            pltpu.VMEM((DIRECT,) + tile, f32),
            pltpu.VMEM((DIRECT,) + tile, f32),
            pltpu.VMEM((2,) + tile, f32),
            pltpu.VMEM((2,) + tile, f32),
            pltpu.VMEM((2,) + tile, f32),
            pltpu.VMEM((2 * ni, pr, dim), f32),
            pltpu.VMEM((pr, dim), f32),
            pltpu.VMEM((ni * no, pr, dim), f32),
            pltpu.VMEM((dim, rows), f32),
            pltpu.VMEM((2,) + tile, f32),
            pltpu.VMEM((2,) + tile, f32),
            pltpu.VMEM((2, 2) + tile, f32),
            pltpu.VMEM((2 * block + (4 * ni - 3) * pr, dim), f32),
            pltpu.SemaphoreType.DMA((14,)),
            pltpu.SemaphoreType.DMA((21,)),
            pltpu.SemaphoreType.REGULAR((2,)),
        ],
        compiler_params=pltpu.CompilerParams(
            collective_id=0, has_side_effects=True, vmem_limit_bytes=66_000_000
        ),
    )(
        sink_len, window_len, codes,
        queries.reshape(rows, dim), key_rows.T, values.T, out_grad.reshape(rows, dim),
    )
    grad_q, grad_k, grad_v = pl.pallas_call(
        store,
        out_shape=(
            jax.ShapeDtypeStruct((rows, dim), f32),
            jax.ShapeDtypeStruct((half, block), f32),
            jax.ShapeDtypeStruct((half, block), f32),
        ),
        in_specs=[vmem] * 2,
        out_specs=(hbm,) * 3,
        scratch_shapes=[pltpu.SemaphoreType.DMA((3,))],
        compiler_params=pltpu.CompilerParams(vmem_limit_bytes=1 << 20),
    )(grad_q, grad_kv)
    return grad_q.reshape(queries.shape), grad_k.T, grad_v.T


def solution(mesh):
    in_specs = (
        P(("inner", "outer"), "head", None),
        P(("inner", "outer"), "head"),
        P(("inner", "outer"), "head"),
        P(("inner", "outer"), "head", None),
        P(),
        P(),
        P(),
    )
    out_specs = (
        P(("inner", "outer"), "head", None),
        P(("inner", "outer"), "head"),
        P(("inner", "outer"), "head"),
    )
    body = functools.partial(shards, mesh.shape["inner"], mesh.shape["outer"])
    return jax.shard_map(body, mesh=mesh, in_specs=in_specs, out_specs=out_specs, check_vma=False)
```
